256 devices in a mesh: pipe: 2 (over x_hi), tensor: 8 (over y, core), seq: 16 (over z, x_lo).
Axes of the slice: x: 4 (x_hi: 2, x_lo: 2; x = x_hi * 2 + x_lo), y: 4, z: 8, core: 2. Of those that a mesh axis runs over, the one named last changes fastest.
Arguments:
- tokens: bfloat16 [2, 2048, 2560], P(None, 'seq', 'tensor'), may hold values from -6 to 6
- prenorm_gain: float32 [2, 2560], P('pipe'), may hold values from 0.5 to 1.5
- gate_weight: bfloat16 [2, 2560, 5120], P('pipe', None, 'tensor'), may hold values from -0.125 to 0.125
- inner_weight: bfloat16 [2, 2560, 5120], P('pipe', None, 'tensor'), may hold values from -0.125 to 0.125
- state_weight: bfloat16 [2, 2560, 256], P('pipe'), may hold values from -0.125 to 0.125
- step_weight: bfloat16 [2, 2560, 80], P('pipe', None, 'tensor'), may hold values from -0.125 to 0.125
- inner_taps: float32 [2, 5, 5120], P('pipe', None, 'tensor'), may hold values from -3 to 3
- state_taps: float32 [2, 5, 256], P('pipe'), may hold values from -3 to 3
- step_bias: float32 [2, 80], P('pipe', 'tensor'), may hold values from -5 to -2
- decay_rate: float32 [2, 80], P('pipe', 'tensor'), may hold values from 0.00048828125 to 1
- skip_scale: float32 [2, 80], P('pipe', 'tensor'), may hold values from 0.5 to 1.5
- inner_gain: float32 [2, 5120], P('pipe', 'tensor'), may hold values from 0.5 to 1.5
- out_weight: bfloat16 [2, 5120, 2560], P('pipe', 'tensor'), may hold values from -0.078125 to 0.078125
Outputs:
- layer_outputs: bfloat16 [2, 2, 2048, 2560], P('pipe', None, 'seq', 'tensor')
The draws below stay inside these ranges and needn't reach their ends.
All inputs are finite; a program needn't handle non-finite values.
Results may differ from the reference program's by a relative error of at most 0.019.
Values may be sent and summed in bfloat16 or wider, within the bound.
No kernel may reach another device: no remote copies, remote signals or barrier semaphores. Data moves between devices by JAX's collectives and lax.ppermute only.
A program may use at most 64 MiB of HBM per device.

```python
import math
import jax
import jax.numpy as jnp
from jax import lax

D = 2560
HEADS = 80
HEADDIM = 64
STATE = 128
KW = 4
BLOCK = 128
MICRO = 2
INNER = 5120
TOKENS = 2048
LAYERS = 2


def block_levels(own_key, extent, cuts, least, top_value):
    level, own = 1.0, jax.random.fold_in(own_key, 6)
    for position, shards_of in cuts:
        steps = jnp.exp(jax.random.uniform(jax.random.fold_in(own, position), (shards_of,), jnp.float32, least / len(cuts), top_value / len(cuts)))
        level = level * jnp.repeat(steps, extent[position] // shards_of).reshape([-1 if axis == position else 1 for axis in range(len(extent))])
    return level


def gaussian(own_key, shape, scale, bound, shards=(), held_as=jnp.bfloat16):
    values = scale * jax.random.normal(own_key, shape, jnp.float32)
    if shards:
        values = values * block_levels(own_key, shape, shards, -0.22, 0.18)
    return jnp.clip(values, -bound, bound).astype(held_as)


def setup_inputs(seed: int = 0) -> dict:
    splits = jax.random.split(jax.random.key(seed), 14)
    return {
        "tokens": gaussian(splits[0], (MICRO, TOKENS, D), 1.0, 6.0, ((1, 16), (2, 8))),
        "prenorm_gain": jnp.clip(1.0 + 0.1 * jax.random.normal(splits[1], (LAYERS, D), jnp.float32), 0.5, 1.5),
        "gate_weight": gaussian(splits[2], (LAYERS, D, INNER), D ** -0.5, 0.125, ((0, 2), (2, 8))),
        "inner_weight": gaussian(splits[3], (LAYERS, D, INNER), D ** -0.5, 0.125, ((0, 2), (2, 8))),
        "state_weight": gaussian(splits[4], (LAYERS, D, 2 * STATE), D ** -0.5, 0.125, ((0, 2),)),
        "step_weight": gaussian(splits[5], (LAYERS, D, HEADS), D ** -0.5, 0.125, ((0, 2), (2, 8))),
        "inner_taps": gaussian(splits[6], (LAYERS, KW + 1, INNER), 0.5, 3.0, ((0, 2), (2, 8)), jnp.float32),
        "state_taps": gaussian(splits[7], (LAYERS, KW + 1, 2 * STATE), 0.5, 3.0, ((0, 2),), jnp.float32),
        "step_bias": jnp.clip(-5.0 + 3.0 * jax.random.uniform(splits[8], (LAYERS, HEADS), jnp.float32) ** block_levels(splits[8], (LAYERS, HEADS), ((0, 2), (1, 8)), -0.2, 0.2), -5.0, -2.0),
        "decay_rate": jnp.clip(jnp.exp(math.log(1.0) - 7.624619 * jax.random.uniform(splits[9], (LAYERS, HEADS), jnp.float32) ** block_levels(splits[9], (LAYERS, HEADS), ((0, 2), (1, 8)), -0.2, 0.2)), 0.00048828125, 1.0),
        "skip_scale": jnp.clip(0.5 + 1.0 * jax.random.uniform(splits[10], (LAYERS, HEADS), jnp.float32) ** block_levels(splits[10], (LAYERS, HEADS), ((0, 2), (1, 8)), -0.2, 0.2), 0.5, 1.5),
        "inner_gain": jnp.clip(1.0 + 0.1 * jax.random.normal(splits[11], (LAYERS, INNER), jnp.float32), 0.5, 1.5),
        "out_weight": gaussian(splits[12], (LAYERS, INNER, D), INNER ** -0.5, 0.078125, ((0, 2), (1, 8))),
    }


EPS = 1e-05

def causal_taps(values, taps):
    width = taps.shape[0] - 1
    length = values.shape[0]
    zeros = jnp.zeros((width - 1, values.shape[1]), values.dtype)
    padded = jnp.concatenate([zeros, values], axis=0).astype(jnp.float32)
    total = jnp.broadcast_to(taps[width][None, :], (length, values.shape[1]))
    for index in range(width):
        total = total + taps[index][None, :] * padded[index:index + length]
    return jax.nn.silu(total).astype(jnp.bfloat16)

def block_terms(inner_block, input_block, output_block, step_block, rate):
    size = step_block.shape[0]
    cumulative = jnp.cumsum(-step_block * rate[None, :], axis=0)
    by_head = cumulative.T
    later = jnp.arange(size)[:, None] >= jnp.arange(size)[None, :]
    decay = jnp.exp(jnp.where(later[None], by_head[:, :, None] - by_head[:, None, :], -jnp.inf))
    scores = jnp.dot(output_block, input_block.T, preferred_element_type=jnp.float32)
    mixing = (scores[None] * decay * step_block.T[:, None, :]).astype(jnp.bfloat16)
    inside = jnp.einsum('hqs,shp->qhp', mixing.astype(jnp.float32), inner_block.astype(jnp.float32))
    weighting = jnp.exp(cumulative[-1:] - cumulative) * step_block
    weighted = (inner_block.astype(jnp.float32) * weighting[:, :, None]).astype(jnp.bfloat16)
    state = jnp.einsum('shp,sn->hpn', weighted.astype(jnp.float32), input_block.astype(jnp.float32))
    return (cumulative, inside, state, jnp.exp(cumulative[-1]))

def state_space(inner_conv, state_conv, step_size, rate, skip):
    length = inner_conv.shape[0]
    count = length // BLOCK
    inner_blocks = inner_conv.reshape(count, BLOCK, HEADS, HEADDIM)
    input_blocks = state_conv[:, :STATE].reshape(count, BLOCK, STATE)
    output_blocks = state_conv[:, STATE:].reshape(count, BLOCK, STATE)
    step_blocks = step_size.reshape(count, BLOCK, HEADS)

    def advance(carried, items):
        inner_block, input_block, output_block, step_block = items
        cumulative, inside, state, decay = block_terms(inner_block, input_block, output_block, step_block, rate)
        across = jnp.exp(cumulative)[:, :, None] * jnp.einsum('qn,hpn->qhp', output_block.astype(jnp.float32), carried, precision=lax.Precision.HIGHEST)
        return (carried * decay[:, None, None] + state, inside + across)
    initial = jnp.zeros((HEADS, HEADDIM, STATE), jnp.float32)
    _, pieces = lax.scan(advance, initial, (inner_blocks, input_blocks, output_blocks, step_blocks))
    mixed = pieces + skip[None, None, :, None] * inner_blocks.astype(jnp.float32)
    return mixed.reshape(length, HEADS * HEADDIM)

def layer(current, prenorm, gate_weight, inner_weight, state_weight, step_weight, inner_taps, state_taps, step_bias, decay_rate, skip_scale, inner_gain, out_weight):
    widened = current.astype(jnp.float32)
    normed_in = (widened * lax.rsqrt(lax.optimization_barrier(jnp.mean(widened * widened, axis=1, keepdims=True)) + EPS) * prenorm).astype(jnp.bfloat16)
    gate_raw = jnp.dot(normed_in, gate_weight, preferred_element_type=jnp.float32).astype(jnp.bfloat16)
    inner_raw = jnp.dot(normed_in, inner_weight, preferred_element_type=jnp.float32).astype(jnp.bfloat16)
    state_raw = jnp.dot(normed_in, state_weight, preferred_element_type=jnp.float32).astype(jnp.bfloat16)
    step_raw = jnp.dot(normed_in, step_weight, preferred_element_type=jnp.float32)
    inner_conv = causal_taps(inner_raw, inner_taps)
    state_conv = causal_taps(state_raw, state_taps)
    step_size = jax.nn.softplus(step_raw + step_bias)
    mixed = state_space(inner_conv, state_conv, step_size, decay_rate, skip_scale)
    gated = mixed * jax.nn.silu(gate_raw.astype(jnp.float32))
    normed = (gated * lax.rsqrt(lax.optimization_barrier(jnp.mean(gated * gated, axis=1, keepdims=True)) + EPS) * inner_gain).astype(jnp.bfloat16)
    summed = jnp.dot(normed, out_weight, preferred_element_type=jnp.float32)
    return (widened + summed).astype(jnp.bfloat16)

def reference(tokens, prenorm_gain, gate_weight, inner_weight, state_weight, step_weight, inner_taps, state_taps, step_bias, decay_rate, skip_scale, inner_gain, out_weight):
    results = []
    for micro in range(MICRO):
        current = tokens[micro]
        per_layer = []
        for depth in range(LAYERS):
            current = layer(current, prenorm_gain[depth], gate_weight[depth], inner_weight[depth], state_weight[depth], step_weight[depth], inner_taps[depth], state_taps[depth], step_bias[depth], decay_rate[depth], skip_scale[depth], inner_gain[depth], out_weight[depth])
            per_layer.append(current)
        results.append(jnp.stack(per_layer))
    return jnp.stack(results, axis=1)
```

```python
import jax
import jax.numpy as jnp
from jax import lax
from jax.sharding import Mesh
from jax.sharding import PartitionSpec as P

BLOCK = 128
INNER = 5120
EPS = 1e-05
SEQ = ("seq_0", "seq_1")
TENSOR = ("chip", "core")
SWAP = [(0, 1), (1, 0)]
F32 = jnp.float32
BF16 = jnp.bfloat16


def ring(size, steps):
    return [(source, (source + steps) % size) for source in range(size)]


def split_bf16(value, count):
    parts = []
    for _ in range(count):
        part = value.astype(BF16)
        parts.append(part)
        value = value - part.astype(F32)
    return parts


def causal_taps(rim, values, taps):
    width = taps.shape[0] - 1
    length = values.shape[1]
    padded = jnp.concatenate([rim, values], axis=1).astype(F32)
    total = taps[width]
    for index in range(width):
        total = total + taps[index] * padded[:, index : index + length]
    return jax.nn.silu(total).astype(BF16)


def gather_rows(piece):
    chip = lax.axis_index("chip")
    count = lax.axis_size("chip")
    pieces = jnp.stack(
        [piece] + [lax.ppermute(piece, "chip", ring(count, k)) for k in range(1, count)]
    )
    own = jnp.concatenate(
        [
            lax.dynamic_index_in_dim(pieces, lax.rem(chip - b + count, count), 0, keepdims=False)
            for b in range(count)
        ],
        axis=1,
    )
    other = lax.ppermute(own, "core", SWAP)
    return jnp.stack([own, other])


def exchange_states(states, decays):
    micros, rows, width = states.shape
    heads = decays.shape[1]
    head_rows = rows // heads
    members = lax.axis_size(SEQ)
    share = rows // members
    member = lax.axis_index(SEQ)
    first = [(s * share) // head_rows for s in range(members)]
    last = [(s * share + share - 1) // head_rows for s in range(members)]
    ends = jnp.stack(
        [
            jnp.stack([decays[:, h] for h in first]),
            jnp.stack([decays[:, h] for h in last]),
        ],
        axis=2,
    )
    ends = ends.reshape(members, micros * 2)
    high, low = split_bf16(ends, 2)
    extra = jnp.concatenate([high, low, high, low], axis=1)
    body = jnp.moveaxis(states.astype(BF16).reshape(micros, members, share, width), 0, 1)
    body = body.reshape(members, micros * share, width)
    sent = jnp.concatenate(
        [body, jnp.broadcast_to(extra[:, :, None], (*extra.shape, width))], axis=1
    )
    arrived = lax.all_to_all(sent, SEQ, 0, 0, tiled=True)
    ends = arrived[:, micros * share :].astype(F32)
    ends = ends[:, : 2 * micros] + ends[:, 2 * micros : 4 * micros]
    ends = ends.reshape(members, micros, 2, width)
    body = arrived[:, : micros * share].reshape(members, micros, share, width).astype(F32)
    row = member * share + lax.broadcasted_iota(jnp.int32, (share, width), 0)
    leading = row // head_rows == member * share // head_rows
    running = jnp.zeros((micros, share, width), F32)
    entering = []
    for s in range(members):
        entering.append(running.astype(BF16).reshape(micros * share, width))
        factor = jnp.where(leading, ends[s, :, 0:1], ends[s, :, 1:2])
        running = factor * running + body[s]
    back = lax.all_to_all(jnp.stack(entering), SEQ, 0, 0, tiled=True)
    back = jnp.moveaxis(back.reshape(members, micros, share, width), 1, 0)
    return back.reshape(micros, rows, width)


def layer(piece, weights):
    (
        prenorm,
        gate_weight,
        inner_weight,
        state_weight,
        step_weight,
        inner_taps,
        state_taps,
        step_bias,
        decay_rate,
        skip_scale,
        inner_gain,
        out_weight,
    ) = weights
    current = gather_rows(piece)
    micros, rows, _ = current.shape
    widened = current.astype(F32)
    normed_in = (
        widened * lax.rsqrt(jnp.mean(widened * widened, axis=2, keepdims=True) + EPS) * prenorm
    ).astype(BF16)
    inner_raw = jnp.dot(normed_in, inner_weight, preferred_element_type=F32).astype(BF16)
    state_raw = jnp.dot(normed_in, state_weight, preferred_element_type=F32).astype(BF16)
    reach = inner_taps.shape[0] - 2
    inner_width = inner_raw.shape[2]
    rim = lax.ppermute(
        jnp.concatenate([inner_raw[:, rows - reach :], state_raw[:, rows - reach :]], axis=2),
        SEQ,
        [(s, s + 1) for s in range(lax.axis_size(SEQ) - 1)],
    )
    step_raw = jnp.dot(normed_in, step_weight, preferred_element_type=F32)
    gate_raw = jnp.dot(normed_in, gate_weight, preferred_element_type=F32).astype(BF16)
    inner_conv = causal_taps(rim[:, :, :inner_width], inner_raw, inner_taps)
    state_conv = causal_taps(rim[:, :, inner_width:], state_raw, state_taps)
    heads = step_bias.shape[0]
    head_size = inner_width // heads
    state_size = state_raw.shape[2] // 2
    step_size = jax.nn.softplus(step_raw + step_bias)
    cumulative = jnp.cumsum(-step_size * decay_rate, axis=1)
    x = inner_conv.reshape(micros, rows, heads, head_size)
    b_map = state_conv[:, :, :state_size]
    c_map = state_conv[:, :, state_size:]
    weighting = jnp.exp(cumulative[:, -1:, :] - cumulative) * step_size
    weighted = (x.astype(F32) * weighting[..., None]).astype(BF16)
    states = jnp.einsum(
        "mrc,mrn->mcn", weighted.reshape(micros, rows, inner_width), b_map, preferred_element_type=F32
    )
    entering = exchange_states(states, jnp.exp(cumulative[:, -1, :]))
    scores = jnp.einsum("mqn,msn->mqs", c_map, b_map, preferred_element_type=F32)
    by_head = jnp.transpose(cumulative, (0, 2, 1))
    later = lax.broadcasted_iota(jnp.int32, (rows, rows), 0) >= lax.broadcasted_iota(
        jnp.int32, (rows, rows), 1
    )
    decay = jnp.exp(jnp.where(later, by_head[:, :, :, None] - by_head[:, :, None, :], -jnp.inf))
    mixing = (
        scores[:, None] * decay * jnp.transpose(step_size, (0, 2, 1))[:, :, None, :]
    ).astype(BF16)
    inside = jnp.einsum("mhqs,mshp->mqhp", mixing, x, preferred_element_type=F32)
    across = jnp.einsum("mqn,mcn->mqc", c_map, entering, preferred_element_type=F32)
    across = across.reshape(micros, rows, heads, head_size) * jnp.exp(cumulative)[..., None]
    mixed = inside + across + skip_scale[:, None] * x.astype(F32)
    gated = mixed.reshape(micros, rows, inner_width) * jax.nn.silu(gate_raw.astype(F32))
    squares = jnp.sum(gated * gated, axis=2)
    scaled = (gated * inner_gain).astype(BF16)
    term = jnp.dot(scaled, out_weight, preferred_element_type=F32).astype(BF16)
    return scatter_rows(piece, term, squares)


def with_squares(term, squares):
    rows, width = term.shape[-2:]
    row = jnp.concatenate(split_bf16(squares, 3))[None]
    row = jnp.pad(row, ((0, 7), (0, width - row.shape[1])))
    return jnp.concatenate([term, row], axis=0)


def from_squares(array, rows):
    row = array[rows].astype(F32)
    return array[:rows].astype(F32), row[:rows] + row[rows : 2 * rows] + row[2 * rows : 3 * rows]


def scatter_rows(piece, term, squares):
    chip = lax.axis_index("chip")
    count = lax.axis_size("chip")
    rows, width = piece.shape
    arrived = lax.ppermute(with_squares(term[1], squares[1]), "core", SWAP)
    other, other_squares = from_squares(arrived, rows)
    total = term[0].astype(F32) + other
    summed_squares = squares[0] + other_squares
    blocks = jnp.moveaxis(total.astype(BF16).reshape(rows, count, width), 1, 0)
    mine = lax.dynamic_index_in_dim(blocks, chip, 0, keepdims=False).astype(F32)
    all_squares = summed_squares
    for k in range(1, count):
        block = lax.dynamic_index_in_dim(blocks, lax.rem(chip + k, count), 0, keepdims=False)
        arrived = lax.ppermute(with_squares(block, summed_squares), "chip", ring(count, k))
        value, value_squares = from_squares(arrived, rows)
        mine = mine + value
        all_squares = all_squares + value_squares
    scale = lax.rsqrt(all_squares / INNER + EPS)
    return (piece.astype(F32) + scale[:, None] * mine).astype(BF16)


def shards(
    tokens,
    prenorm_gain,
    gate_weight,
    inner_weight,
    state_weight,
    step_weight,
    inner_taps,
    state_taps,
    step_bias,
    decay_rate,
    skip_scale,
    inner_gain,
    out_weight,
):
    weights = (
        prenorm_gain[0],
        gate_weight[0],
        inner_weight[0],
        state_weight[0],
        step_weight[0],
        inner_taps[0],
        state_taps[0],
        step_bias[0],
        decay_rate[0],
        skip_scale[0],
        inner_gain[0],
        out_weight[0],
    )
    sections = lax.axis_size("pipe")
    section = lax.axis_index("pipe")
    core = lax.axis_index("core")
    width = tokens.shape[2]
    mine = jnp.where(core == 0, tokens[0], tokens[1])
    given = lax.ppermute(jnp.where(core == 0, tokens[1], tokens[0]), "core", SWAP)
    piece = jnp.where(
        core == 0, jnp.concatenate([mine, given], 1), jnp.concatenate([given, mine], 1)
    )
    kept = None
    for turn in range(sections):
        own = layer(piece, weights)
        kept = own if turn == 0 else jnp.where(section == turn, own, kept)
        if turn + 1 < sections:
            piece = lax.ppermute(own, "pipe", [(s, s + 1) for s in range(sections - 1)])
    left, right = kept[:, :width], kept[:, width:]
    held = jnp.where(core == 0, left, right)
    given = lax.ppermute(jnp.where(core == 0, right, left), "core", SWAP)
    return jnp.where(core == 0, jnp.stack([held, given]), jnp.stack([given, held]))[None]


def solution(mesh):
    torus = Mesh(
        mesh.devices.reshape(mesh.shape["pipe"], mesh.shape["tensor"] // 2, 2, 8, 2),
        ("pipe", "chip", "core", "seq_0", "seq_1"),
    )
    return jax.shard_map(
        shards,
        mesh=torus,
        in_specs=(
            P(None, SEQ, TENSOR),
            P("pipe", None),
            P("pipe", None, TENSOR),
            P("pipe", None, TENSOR),
            P("pipe", None, None),
            P("pipe", None, TENSOR),
            P("pipe", None, TENSOR),
            P("pipe", None, None),
            P("pipe", TENSOR),
            P("pipe", TENSOR),
            P("pipe", TENSOR),
            P("pipe", TENSOR),
            P("pipe", TENSOR, None),
        ),
        out_specs=P("pipe", None, SEQ, TENSOR),
        check_vma=False,
    )
```

```python
import jax
import jax.numpy as jnp
from jax import lax
from jax.experimental import pallas as pl
from jax.experimental.pallas import tpu as pltpu
from jax.sharding import Mesh
from jax.sharding import PartitionSpec as P

BLOCK = 128
INNER = 5120
EPS = 1e-05
EDGE = 8
SEQ = ("seq_0", "seq_1")
TENSOR = ("chip", "core")
SWAP = [(0, 1), (1, 0)]
F32 = jnp.float32
BF16 = jnp.bfloat16
VMEM = pl.BlockSpec(memory_space=pltpu.VMEM)
SMEM = pl.BlockSpec(memory_space=pltpu.SMEM)
HBM = pl.BlockSpec(memory_space=pltpu.MemorySpace.HBM)


def ring(size, steps):
    return [(source, (source + steps) % size) for source in range(size)]


def split_bf16(value, count):
    parts = []
    for _ in range(count):
        part = value.astype(BF16)
        parts.append(part)
        value = value - part.astype(F32)
    return parts


def local(body, args, outs, scalars=0, weights=0, scratch=(), mib=16, flops=1 << 28):
    first = len(args) - weights
    args = [
        pltpu.with_memory_space_constraint(arg, pltpu.MemorySpace.HBM) if index >= first else arg
        for index, arg in enumerate(args)
    ]
    return pl.pallas_call(
        body,
        out_shape=[jax.ShapeDtypeStruct(shape, kind) for shape, kind in outs],
        in_specs=[SMEM] * scalars + [VMEM] * (len(args) - scalars - weights) + [HBM] * weights,
        out_specs=[VMEM] * len(outs),
        cost_estimate=pl.CostEstimate(flops=flops, transcendentals=0, bytes_accessed=1 << 22),
        name=body.__name__,
        scratch_shapes=list(scratch),
        compiler_params=pltpu.CompilerParams(vmem_limit_bytes=mib << 20),
    )(*args)


def fetch(source, target, semaphores):
    parts = semaphores.shape[0]
    size = source.shape[0] // parts
    copies = [
        pltpu.make_async_copy(
            source.at[pl.ds(part * size, size)],
            target.at[pl.ds(part * size, size)],
            semaphores.at[part],
        )
        for part in range(parts)
    ]
    for copy in copies:
        copy.start()
    return copies


def room(weight, parts):
    return [pltpu.VMEM(weight.shape, weight.dtype), pltpu.SemaphoreType.DMA((parts,))]


def dot(a, b, dims=((1,), (0,))):
    return lax.dot_general(a, b, (dims, ((), ())), preferred_element_type=F32)


def sigmoid(value):
    return 1.0 / (1.0 + jnp.exp(-value))


def iota(shape, dim):
    return lax.broadcasted_iota(jnp.int32, shape, dim)


def spread(heads, width):
    size = width // heads
    lane, head = iota((heads, width), 1), iota((heads, width), 0)
    return jnp.where((lane >= head * size) & (lane < (head + 1) * size), 1.0, 0.0).astype(BF16)


def over_channels(value, picks):
    return sum(dot(part, picks) for part in split_bf16(value, 3))


def convolve(rim, values, taps):
    width = taps.shape[0] - 1
    length = values.shape[0]
    padded = jnp.concatenate([rim, values], axis=0).astype(F32)
    lead = rim.shape[0] - width + 1
    total = taps[width]
    for index in range(width):
        total = total + taps[index] * padded[lead + index : lead + index + length]
    return (total * sigmoid(total)).astype(BF16)


def enter(chip_ref, *refs):
    count = (len(refs) - 19) // 2
    sides = refs[:count], refs[count : 2 * count]
    gain, step_w, inner_taps, state_taps, bias, rate, state_hbm, inner_hbm = refs[2 * count :][:8]
    normed, x, maps, steps, sums, sent, tails = refs[2 * count + 8 :][:7]
    state_w, state_sems, inner_w, inner_sems = refs[2 * count + 15 :]
    state_copies = fetch(state_hbm, state_w, state_sems)
    inner_copies = fetch(inner_hbm, inner_w, inner_sems)
    chip = chip_ref[0]
    rows, width = x.shape[1:]
    block = gain.shape[2]
    edge = sides[0][0].shape[0] - rows
    heads = bias.shape[1]
    n = maps.shape[2] // 2
    for side, pieces in enumerate(sides):
        squares = jnp.zeros((rows + edge, 128), F32)
        for piece in pieces:
            value = piece[...].astype(F32)
            value = value * value
            for tile in range(block // 128):
                squares = squares + value[:, tile * 128 : (tile + 1) * 128]
        scale = lax.rsqrt(jnp.sum(squares, axis=1, keepdims=True) / (count * block) + EPS)
        for k, piece in enumerate(pieces):
            b = lax.rem(chip - k + count, count)
            value = piece[...].astype(F32) * scale * gain[b]
            normed[b, side * rows : (side + 1) * rows, :] = value[edge:].astype(BF16)
            tails[b, side * edge : (side + 1) * edge, :] = value[:edge]

    def times(weight, copies):
        main, tail = 0.0, 0.0
        for b in range(count):
            copies[b].wait()
            part = weight[b * block : (b + 1) * block, :]
            main = main + dot(normed[b], part)
            tail = tail + dot(tails[b].astype(BF16), part)
        return main, tail

    raw = jnp.zeros((2 * rows, heads), F32)
    for b in range(count):
        raw = raw + dot(normed[b], step_w[:, b * block : (b + 1) * block], ((1,), (1,)))
    raw = raw + bias[...]
    step_all = jnp.maximum(raw, 0.0) + jnp.log1p(jnp.exp(-jnp.abs(raw)))
    state, state_tail = times(state_w, state_copies)
    inner, inner_tail = times(inner_w, inner_copies)
    lower = (iota((rows, rows), 0) >= iota((rows, rows), 1)).astype(BF16)
    picks = spread(heads, width)
    for m in range(2):
        span = slice(m * rows, (m + 1) * rows)
        ends = slice(m * edge, (m + 1) * edge)
        xm = convolve(
            inner_tail[ends].astype(BF16).astype(F32),
            inner[span].astype(BF16).astype(F32),
            inner_taps,
        )
        sm = convolve(
            state_tail[ends].astype(BF16).astype(F32),
            state[span].astype(BF16).astype(F32),
            state_taps,
        )
        x[m] = xm
        maps[m] = sm
        step = step_all[span]
        total = -sum(dot(lower, part) for part in split_bf16(step * rate[...], 3))
        last = total[rows - 1 :]
        steps[m] = step
        sums[m] = total
        weighting = over_channels(jnp.exp(last - total) * step, picks)
        weighted = (xm.astype(F32) * weighting).astype(BF16)
        sent[span, :width] = dot(sm[:, :n], weighted, ((0,), (0,))).astype(BF16)
        high, low = split_bf16(jnp.exp(last), 2)
        row = iota((rows, heads), 0) % 16
        ends = jnp.where(row == 0, high.astype(F32), low.astype(F32))
        ends = jnp.concatenate([ends, jnp.zeros((rows, sent.shape[1] - width - heads), F32)], 1)
        sent[span, width:] = ends.astype(BF16)


def gate_project(normed, gate_hbm, gate, gate_w, gate_sems):
    count, _, width = normed.shape
    copies = fetch(gate_hbm, gate_w, gate_sems)
    total = jnp.zeros(gate.shape, F32)
    for block in range(count):
        copies[block].wait()
        total = total + dot(normed[block], gate_w[block * width : (block + 1) * width, :])
    gate[...] = (total.astype(BF16).astype(F32) * sigmoid(total.astype(BF16).astype(F32))).astype(
        gate.dtype
    )


def local_mixing(x, maps, steps, sums, gate, skip, base, ahead):
    micros, rows, width = x.shape
    heads = skip.shape[1]
    size = width // heads
    pair = 128 // size
    n = maps.shape[2] // 2
    picks = spread(heads, width)
    skips = over_channels(jnp.broadcast_to(skip[...], (8, heads)), picks)[:1]
    later = iota((rows, rows), 0) >= iota((rows, rows), 1)
    lane = iota((rows, pair * size), 1)
    for m in range(micros):
        maps_m, sums_m, steps_m = maps[m], sums[m], steps[m]
        scores = dot(maps_m[:, n:], maps_m[:, :n], ((1,), (1,)))
        fill = jnp.zeros((rows, 128 - heads), F32)
        sums_t = jnp.transpose(jnp.concatenate([sums_m, fill], 1))
        steps_t = jnp.transpose(jnp.concatenate([steps_m, fill], 1))
        for g in range(heads // pair):
            span = slice(g * pair * size, (g + 1) * pair * size)
            xg = x[m, :, span]
            left, right = [], []
            for j in range(pair):
                h = g * pair + j
                gap = sums_m[:, h : h + 1] - sums_t[h : h + 1, :]
                decay = jnp.exp(jnp.where(later, gap, -jnp.inf))
                left.append((scores * decay * steps_t[h : h + 1, :]).astype(BF16))
                right.append(
                    jnp.where((lane >= j * size) & (lane < (j + 1) * size), xg, jnp.zeros_like(xg))
                )
            inside = dot(jnp.concatenate(left, 1), jnp.concatenate(right, 0))
            silu = gate[m * rows : (m + 1) * rows, span]
            base[m, :, span] = (inside + skips[:, span] * xg.astype(F32)) * silu
        ahead[m] = over_channels(jnp.exp(sums_m), picks) * gate[m * rows : (m + 1) * rows]


def scan_states(arrived, back, heads=10):
    members, rows, width = back.shape
    picks = spread(128, 128 * (width // heads))[:, :width]
    ends = arrived[:, :, width:].reshape(members * rows, arrived.shape[2] - width)
    factors = dot(ends, picks)
    running = jnp.zeros((rows, width), F32)
    for s in range(members):
        back[s] = running.astype(BF16)
        factor = factors[s * rows : s * rows + 1] + factors[s * rows + 1 : s * rows + 2]
        running = running * factor + arrived[s, :, :width].astype(F32)


def squares_rows(squares):
    rows = squares.shape[0]
    lane = iota((rows, 128), 1)
    block = jnp.zeros((rows, 128), F32)
    for index, part in enumerate(split_bf16(squares, 3)):
        block = jnp.where(lane == index, part.astype(F32), block)
    return jnp.transpose(block)[:8]


def output_term(m, base, ahead, maps, entering, gain, out_hbm, term, out_w, out_sems):
    n = maps.shape[2] // 2
    count, tall, width = term.shape
    (copy,) = fetch(out_hbm, out_w, out_sems)
    rows = base.shape[1]
    across = dot(maps[m, :, n:], entering[m])
    gated = base[m] + across * ahead[m]
    squares = jnp.sum(gated * gated, axis=1, keepdims=True)
    scaled = (gated * gain[...]).astype(BF16)
    block = squares_rows(squares)
    block = jnp.concatenate([block, jnp.zeros((8, width - 128), F32)], 1).astype(term.dtype)
    copy.wait()
    for b in range(count):
        value = dot(scaled, out_w[:, b * width : (b + 1) * width])
        term[b, :rows] = value.astype(term.dtype)
        term[b, rows:] = block


def other_term(*refs):
    output_term(1, *refs)


def own_term(*refs):
    output_term(0, *refs)


def merge_cores(chip_ref, mine, arrived, kept, *sent):
    count, tall, width = mine.shape
    rows = tall - 8
    chip = chip_ref[0]
    kept[:rows] = mine[chip, :rows] + arrived[chip, :rows].astype(F32)
    both = jnp.sum(mine[0, rows:] + arrived[0, rows:].astype(F32), axis=0, keepdims=True)
    row = iota((8, width), 0)
    kept[rows:] = jnp.where(row == 0, both, 0.0)
    block = jnp.zeros((8, width), F32)
    for index, part in enumerate(split_bf16(both, 3)):
        block = jnp.where(row == index, part.astype(F32), block)
    for k in range(1, count):
        b = lax.rem(chip + k, count)
        sent[k - 1][:rows] = (mine[b, :rows] + arrived[b, :rows].astype(F32)).astype(BF16)
        sent[k - 1][rows:] = block.astype(BF16)


def finish(piece, kept, *refs):
    arrived, result = refs[:-1], refs[-1]
    rows = piece.shape[0]
    total = kept[:rows]
    squares = kept[rows:, :128]
    for part in arrived:
        total = total + part[:rows].astype(F32)
        squares = squares + part[rows:, :128].astype(F32)
    squares = jnp.broadcast_to(jnp.sum(squares, axis=0, keepdims=True), (rows, 128))
    scale = lax.rsqrt(jnp.transpose(squares) / INNER + EPS)
    for tile in range(piece.shape[1] // 128):
        span = slice(tile * 128, (tile + 1) * 128)
        result[:, span] = (piece[:, span].astype(F32) + scale * total[:, span]).astype(BF16)


def layer(piece, edge, weights):
    (
        prenorm,
        gate_weight,
        inner_weight,
        state_weight,
        step_weight,
        inner_taps,
        state_taps,
        step_bias,
        decay_rate,
        skip_scale,
        inner_gain,
        out_weight,
    ) = weights
    chip = lax.axis_index("chip").reshape(1)
    count = lax.axis_size("chip")
    members = lax.axis_size(SEQ)
    rows, block = piece.shape
    tall = 2 * rows
    width = inner_weight.shape[1]
    maps_width = state_weight.shape[1]
    heads = step_weight.shape[1]
    spread_rows = jnp.concatenate([edge, piece], axis=0)
    own = [spread_rows] + [
        lax.ppermute(spread_rows, "chip", ring(count, k)) for k in range(1, count)
    ]
    other = [lax.ppermute(part, "core", SWAP) for part in own]
    normed, x, maps, steps, sums, sent = local(
        enter,
        [
            chip,
            *own,
            *other,
            prenorm.reshape(count, 1, block),
            step_weight.T,
            inner_taps[:, None],
            state_taps[:, None],
            step_bias[None],
            decay_rate[None],
            state_weight,
            inner_weight,
        ],
        [
            ((count, tall, block), BF16),
            ((2, rows, width), BF16),
            ((2, rows, maps_width), BF16),
            ((2, rows, heads), F32),
            ((2, rows, heads), F32),
            ((tall, width + 128), BF16),
        ],
        scalars=1,
        weights=2,
        scratch=[
            pltpu.VMEM((count, 2 * edge.shape[0], block), F32),
            *room(state_weight, count),
            *room(inner_weight, count),
        ],
    )
    with jax.named_scope("forth"):
        arrived = lax.all_to_all(
            sent.reshape(members, tall // members, -1), SEQ, 0, 0, tiled=True
        )
    (gate,) = local(
        gate_project,
        [normed, gate_weight],
        [((tall, width), F32)],
        weights=1,
        scratch=room(gate_weight, count),
    )
    base, ahead = local(
        local_mixing,
        [x, maps, steps, sums, gate, skip_scale[None]],
        [((2, rows, width), F32), ((2, rows, width), F32)],
    )
    (back,) = local(scan_states, [arrived], [((members, tall // members, width), BF16)])
    back = lax.all_to_all(back, SEQ, 0, 0, tiled=True)
    entering = back.reshape(2, rows, width)
    common = [base, ahead, maps, entering, inner_gain[None], out_weight]
    (given,) = local(
        other_term, common, [((count, rows + 8, block), BF16)], weights=1, scratch=room(out_weight, 1)
    )
    taken = lax.ppermute(given, "core", SWAP)
    (mine,) = local(
        own_term, common, [((count, rows + 8, block), F32)], weights=1, scratch=room(out_weight, 1)
    )
    kept, *leaving = local(
        merge_cores,
        [chip, mine, taken],
        [((rows + 8, block), F32)] + [((rows + 8, block), BF16)] * (count - 1),
        scalars=1,
    )
    parts = [lax.ppermute(part, "chip", ring(count, k + 1)) for k, part in enumerate(leaving)]
    return local(finish, [piece, kept, *parts], [((rows, block), BF16)])[0]


def shards(
    tokens,
    prenorm_gain,
    gate_weight,
    inner_weight,
    state_weight,
    step_weight,
    inner_taps,
    state_taps,
    step_bias,
    decay_rate,
    skip_scale,
    inner_gain,
    out_weight,
):
    weights = (
        prenorm_gain[0],
        gate_weight[0],
        inner_weight[0],
        state_weight[0],
        step_weight[0],
        inner_taps[0],
        state_taps[0],
        step_bias[0],
        decay_rate[0],
        skip_scale[0],
        inner_gain[0],
        out_weight[0],
    )
    sections = lax.axis_size("pipe")
    section = lax.axis_index("pipe")
    core = lax.axis_index("core")
    width = tokens.shape[2]
    members = lax.axis_size(SEQ)
    mine = jnp.where(core == 0, tokens[0], tokens[1])
    theirs = jnp.where(core == 0, tokens[1], tokens[0])
    given = lax.ppermute(theirs, "core", SWAP)
    mine_edge = lax.ppermute(mine[-EDGE:], SEQ, [(s, s + 1) for s in range(members - 1)])
    given_edge = lax.ppermute(
        theirs[-EDGE:],
        ("core", *SEQ),
        [
            (c * members + s, (1 - c) * members + s + 1)
            for c in range(2)
            for s in range(members - 1)
        ],
    )

    def joined(left, right):
        return jnp.where(
            core == 0, jnp.concatenate([left, right], 1), jnp.concatenate([right, left], 1)
        )

    piece, edge = joined(mine, given), joined(mine_edge, given_edge)
    kept = None
    for turn in range(sections):
        own = layer(piece, edge, weights)
        kept = own if turn == 0 else jnp.where(section == turn, own, kept)
        if turn + 1 < sections:
            piece = lax.ppermute(own, "pipe", [(s, s + 1) for s in range(sections - 1)])
            edge = lax.ppermute(
                own[-EDGE:],
                ("pipe", *SEQ),
                [
                    (p * members + s, (p + 1) * members + s + 1)
                    for p in range(sections - 1)
                    for s in range(members - 1)
                ],
            )
    left, right = kept[:, :width], kept[:, width:]
    held = jnp.where(core == 0, left, right)
    given = lax.ppermute(jnp.where(core == 0, right, left), "core", SWAP)
    return jnp.where(core == 0, jnp.stack([held, given]), jnp.stack([given, held]))[None]


def solution(mesh):
    torus = Mesh(
        mesh.devices.reshape(mesh.shape["pipe"], mesh.shape["tensor"] // 2, 2, 8, 2),
        ("pipe", "chip", "core", "seq_0", "seq_1"),
    )
    return jax.shard_map(
        shards,
        mesh=torus,
        in_specs=(
            P(None, SEQ, TENSOR),
            P("pipe", None),
            P("pipe", None, TENSOR),
            P("pipe", None, TENSOR),
            P("pipe", None, None),
            P("pipe", None, TENSOR),
            P("pipe", None, TENSOR),
            P("pipe", None, None),
            P("pipe", TENSOR),
            P("pipe", TENSOR),
            P("pipe", TENSOR),
            P("pipe", TENSOR),
            P("pipe", TENSOR, None),
        ),
        out_specs=P("pipe", None, SEQ, TENSOR),
        check_vma=False,
    )
```

```python
import jax
import jax.numpy as jnp
from jax import lax
from jax.experimental import pallas as pl
from jax.experimental.pallas import tpu as pltpu
from jax.sharding import Mesh
from jax.sharding import PartitionSpec as P

INNER = 5120
EPS = 1e-05
EDGE = 8
NEAR = (0,)
FAR = (2, 1, 3)
SEQ = ("seq_0", "seq_1")
TENSOR = ("chip", "core")
SWAP = [(0, 1), (1, 0)]
F32 = jnp.float32
BF16 = jnp.bfloat16
VMEM = pl.BlockSpec(memory_space=pltpu.VMEM)
SMEM = pl.BlockSpec(memory_space=pltpu.SMEM)
HBM = pl.BlockSpec(memory_space=pltpu.MemorySpace.HBM)


def ring(size, steps):
    return [(source, (source + steps) % size) for source in range(size)]


def split_bf16(value, count):
    parts = []
    for _ in range(count):
        part = value.astype(BF16)
        parts.append(part)
        value = value - part.astype(F32)
    return parts


def local(body, args, outs, scalars=0, weights=0, scratch=(), mib=16, flops=1 << 28):
    first = len(args) - weights
    args = [
        pltpu.with_memory_space_constraint(arg, pltpu.MemorySpace.HBM) if index >= first else arg
        for index, arg in enumerate(args)
    ]
    return pl.pallas_call(
        body,
        out_shape=[jax.ShapeDtypeStruct(shape, kind) for shape, kind in outs],
        in_specs=[SMEM] * scalars + [VMEM] * (len(args) - scalars - weights) + [HBM] * weights,
        out_specs=[VMEM] * len(outs),
        cost_estimate=pl.CostEstimate(flops=flops, transcendentals=0, bytes_accessed=1 << 22),
        scratch_shapes=list(scratch),
        compiler_params=pltpu.CompilerParams(vmem_limit_bytes=mib << 20),
    )(*args)


def fetch(source, target, semaphores, blocks=None):
    parts = semaphores.shape[0]
    size = target.shape[0] // parts
    copies = [
        pltpu.make_async_copy(
            source.at[pl.ds((part if blocks is None else blocks[part]) * size, size)],
            target.at[pl.ds(part * size, size)],
            semaphores.at[part],
        )
        for part in range(parts)
    ]
    for copy in copies:
        copy.start()
    return copies


def blocks_of(steps):
    chip, count = lax.axis_index("chip"), 4
    return [lax.rem(chip - step + count, count) for step in steps]


def fetch_columns(source, target, semaphores):
    parts = semaphores.shape[0]
    size = target.shape[1] // parts
    copies = [
        pltpu.make_async_copy(
            source.at[:, pl.ds(part * size, size)],
            target.at[:, pl.ds(part * size, size)],
            semaphores.at[part],
        )
        for part in range(parts)
    ]
    for copy in copies:
        copy.start()
    return copies


def room(weight, parts, rows=None):
    shape = (rows or weight.shape[0], weight.shape[1])
    return [pltpu.VMEM(shape, weight.dtype), pltpu.SemaphoreType.DMA((parts,))]


def dot(a, b, dims=((1,), (0,))):
    return lax.dot_general(a, b, (dims, ((), ())), preferred_element_type=F32)


def sigmoid(value):
    return 1.0 / (1.0 + jnp.exp(-value))


def iota(shape, dim):
    return lax.broadcasted_iota(jnp.int32, shape, dim)


def spread(heads, width, copies=1):
    size = width // heads
    lane, head = iota((heads * copies, width), 1), iota((heads * copies, width), 0) % heads
    return jnp.where((lane >= head * size) & (lane < (head + 1) * size), 1.0, 0.0).astype(BF16)


def over_channels(value, width):
    parts = [part.astype(F32) for part in split_bf16(value, 3)]
    return dot(jnp.concatenate(parts, 1).astype(BF16), spread(value.shape[1], width, 3))


def convolve(rim, values, taps):
    width = taps.shape[0] - 1
    length = values.shape[0]
    padded = jnp.concatenate([rim, values], axis=0).astype(F32)
    lead = rim.shape[0] - width + 1
    total = taps[width]
    for index in range(width):
        total = total + taps[index] * padded[lead + index : lead + index + length]
    return (total * sigmoid(total)).astype(BF16)


def place(piece, gain, scaled, side, edge):
    rows = piece.shape[0] - edge
    value = piece[...].astype(F32)
    square = value * value
    squares = 0.0
    for tile in range(piece.shape[1] // 128):
        squares = squares + square[:, tile * 128 : (tile + 1) * 128]
    value = value * gain
    scaled[side * rows : (side + 1) * rows, :] = value[edge:].astype(BF16)
    return squares, value[:edge]


def columns(array, b, width):
    return array[:, pl.ds(pl.multiple_of(b * width, width), width)]


def multiply(scaled, part, step_w, state_w, inner_w, copies):
    block = scaled.shape[1]
    span = slice(part * block, (part + 1) * block)
    value = scaled[...]
    step = dot(value, step_w, ((1,), (1,)))
    copies[0][part].wait()
    state = dot(value, state_w[span, :])
    copies[1][part].wait()
    return step, state, dot(value, inner_w[span, :])


def enter_near(*refs):
    count = len(NEAR)
    sides = refs[:count], refs[count : 2 * count]
    gain, step_w, state_hbm, inner_hbm = refs[2 * count :][:4]
    scaled, squares, step, state, inner = refs[2 * count + 4 :][:5]
    state_w, state_sems, inner_w, inner_sems = refs[2 * count + 9 :]
    blocks = blocks_of(NEAR)
    copies = fetch(state_hbm, state_w, state_sems, blocks), fetch(
        inner_hbm, inner_w, inner_sems, blocks
    )
    edge = EDGE
    rows = sides[0][0].shape[0] - edge
    width = sides[0][0].shape[1]
    sums = [0.0, 0.0]
    totals = [0.0, 0.0, 0.0]
    for k, b in enumerate(blocks):
        tails = []
        for side in range(2):
            part, tail = place(sides[side][k], gain[b], scaled.at[k], side, edge)
            sums[side] = sums[side] + part
            tails.append(tail)
        scaled[k, 2 * rows :, :] = jnp.concatenate(tails).astype(BF16)
        parts = multiply(scaled.at[k], k, columns(step_w, b, width), state_w, inner_w, copies)
        totals = [total + part for total, part in zip(totals, parts)]
    for side in range(2):
        squares[side * rows : (side + 1) * rows, :] = sums[side][edge:]
        squares[2 * rows + side * edge : 2 * rows + (side + 1) * edge, :] = sums[side][:edge]
    step[...], state[...], inner[...] = totals


def enter_far(*refs):
    count = len(FAR)
    sides = refs[:count], refs[count : 2 * count]
    squares_in, step_in, state_in, inner_in = refs[2 * count :][:4]
    refs = refs[2 * count + 4 :]
    gain, step_w, inner_taps, state_taps, bias, rate, state_hbm, inner_hbm = refs[:8]
    scaled, scales, x, maps, steps, sums, sent = refs[8:15]
    state_w, state_sems, inner_w, inner_sems = refs[15:]
    blocks = blocks_of(FAR)
    copies = fetch(state_hbm, state_w, state_sems, blocks), fetch(
        inner_hbm, inner_w, inner_sems, blocks
    )
    edge = EDGE
    rows, width = x.shape[1:]
    block = sides[0][0].shape[1]
    heads = bias.shape[1]
    n = maps.shape[2] // 2
    found = [0.0, 0.0]
    for k, b in enumerate(blocks):
        tails = []
        for side in range(2):
            part, tail = place(sides[side][k], gain[b], scaled.at[k], side, edge)
            found[side] = found[side] + part
            tails.append(tail)
        scaled[k, 2 * rows :, :] = jnp.concatenate(tails).astype(BF16)
    found = jnp.concatenate([found[0][edge:], found[1][edge:], found[0][:edge], found[1][:edge]])
    squares = jnp.sum(squares_in[...] + found, axis=1, keepdims=True)
    scale = lax.rsqrt(squares / (len(NEAR + FAR) * block) + EPS)
    scales[...] = jnp.broadcast_to(scale[: 2 * rows], scales.shape)
    totals = [step_in[...], state_in[...], inner_in[...]]
    for k, b in enumerate(blocks):
        parts = multiply(scaled.at[k], k, columns(step_w, b, block), state_w, inner_w, copies)
        totals = [total + part for total, part in zip(totals, parts)]
    step, state, inner = totals
    raw = (step * scale)[: 2 * rows] + bias[...]
    step_all = jnp.maximum(raw, 0.0) + jnp.log1p(jnp.exp(-jnp.abs(raw)))
    state = (state * scale).astype(BF16).astype(F32)
    inner = (inner * scale).astype(BF16).astype(F32)
    lower = (iota((rows, rows), 0) >= iota((rows, rows), 1)).astype(BF16)
    for m in range(2):
        span = slice(m * rows, (m + 1) * rows)
        ends = slice(2 * rows + m * edge, 2 * rows + (m + 1) * edge)
        sm = convolve(state[ends], state[span], state_taps)
        xm = convolve(inner[ends], inner[span], inner_taps)
        x[m] = xm
        maps[m] = sm
        step = step_all[span]
        total = -sum(dot(lower, part) for part in split_bf16(step * rate[...], 3))
        last = total[rows - 1 :]
        steps[m] = step
        sums[m] = total
        weighting = over_channels(jnp.exp(last - total) * step, width)
        weighted = (xm.astype(F32) * weighting).astype(BF16)
        sent[span, :width] = dot(sm[:, :n], weighted, ((0,), (0,))).astype(BF16)
        high, low = split_bf16(jnp.exp(last), 2)
        row = iota((rows, heads), 0) % 16
        ends = jnp.where(row == 0, high.astype(F32), low.astype(F32))
        ends = jnp.concatenate([ends, jnp.zeros((rows, sent.shape[1] - width - heads), F32)], 1)
        sent[span, width:] = ends.astype(BF16)


def gate_project(near, far, scales, gate_hbm, gate, gate_w, gate_sems):
    copies = fetch(gate_hbm, gate_w, gate_sems, blocks_of(NEAR + FAR))
    rows, width = gate.shape
    block = far.shape[2]
    total = 0.0
    for part in range(len(NEAR + FAR)):
        scaled = near[part, :rows] if part < len(NEAR) else far[part - len(NEAR), :rows]
        copies[part].wait()
        total = total + dot(scaled, gate_w[part * block : (part + 1) * block, :])
    for tile in range(width // 128):
        span = slice(tile * 128, (tile + 1) * 128)
        value = (total[:, span] * scales[...]).astype(BF16).astype(F32)
        gate[:, span] = value * sigmoid(value)


def local_mixing(x, maps, steps, sums, gate, skip, base, ahead):
    micros, rows, width = x.shape
    heads = skip.shape[1]
    size = width // heads
    pair = 128 // size
    n = maps.shape[2] // 2
    skips = over_channels(jnp.broadcast_to(skip[...], (8, heads)), width)[:1]
    later = iota((rows, rows), 0) >= iota((rows, rows), 1)
    lane = iota((rows, pair * size), 1)
    for m in range(micros):
        maps_m, sums_m, steps_m = maps[m], sums[m], steps[m]
        scores = dot(maps_m[:, n:], maps_m[:, :n], ((1,), (1,)))
        fill = jnp.zeros((rows, 128 - heads), F32)
        sums_t = jnp.transpose(jnp.concatenate([sums_m, fill], 1))
        steps_t = jnp.transpose(jnp.concatenate([steps_m, fill], 1))
        for g in range(heads // pair):
            span = slice(g * pair * size, (g + 1) * pair * size)
            xg = x[m, :, span]
            left, right = [], []
            for j in range(pair):
                h = g * pair + j
                gap = sums_m[:, h : h + 1] - sums_t[h : h + 1, :]
                decay = jnp.exp(jnp.where(later, gap, -jnp.inf))
                left.append((scores * decay * steps_t[h : h + 1, :]).astype(BF16))
                right.append(
                    jnp.where((lane >= j * size) & (lane < (j + 1) * size), xg, jnp.zeros_like(xg))
                )
            inside = dot(jnp.concatenate(left, 1), jnp.concatenate(right, 0))
            silu = gate[m * rows : (m + 1) * rows, span]
            base[m, :, span] = (inside + skips[:, span] * xg.astype(F32)) * silu
        ahead[m] = over_channels(jnp.exp(sums_m), width) * gate[m * rows : (m + 1) * rows]


def scan_states(arrived, back, heads=10):
    members, rows, width = back.shape
    picks = spread(128, 128 * (width // heads))[:, :width]
    ends = arrived[:, :, width:].reshape(members * rows, arrived.shape[2] - width)
    factors = dot(ends, picks)
    running = jnp.zeros((rows, width), F32)
    for s in range(members):
        back[s] = running.astype(BF16)
        factor = factors[s * rows : s * rows + 1] + factors[s * rows + 1 : s * rows + 2]
        running = running * factor + arrived[s, :, :width].astype(F32)


def squares_rows(squares):
    rows = squares.shape[0]
    lane = iota((rows, 128), 1)
    block = jnp.zeros((rows, 128), F32)
    for index, part in enumerate(split_bf16(squares, 3)):
        block = jnp.where(lane == index, part.astype(F32), block)
    return jnp.transpose(block)[:8]


def output_terms(base, ahead, maps, entering, gain, out_hbm, mine, given, out_w, out_sems):
    n = maps.shape[2] // 2
    count, _, width = mine.shape
    copies = fetch_columns(out_hbm, out_w, out_sems)
    rows = base.shape[1]
    scaled = []
    for m, term in enumerate((mine, given)):
        across = dot(maps[m, :, n:], entering[m])
        gated = base[m] + across * ahead[m]
        squares = jnp.sum(gated * gated, axis=1, keepdims=True)
        scaled.append((gated * gain[...]).astype(BF16))
        block = squares_rows(squares)
        block = jnp.concatenate([block, jnp.zeros((8, width - 128), F32)], 1).astype(term.dtype)
        for b in range(count):
            term[b, rows:] = block
    scaled = jnp.concatenate(scaled)
    for b in range(count):
        copies[b].wait()
        value = dot(scaled, out_w[:, b * width : (b + 1) * width])
        mine[b, :rows] = value[:rows].astype(mine.dtype)
        given[b, :rows] = value[rows:].astype(given.dtype)


def merge_cores(chip_ref, mine, arrived, kept, *sent):
    count, tall, width = mine.shape
    rows = tall - 8
    chip = chip_ref[0]
    kept[:rows] = mine[chip, :rows].astype(F32) + arrived[chip, :rows].astype(F32)
    both = jnp.sum(mine[0, rows:].astype(F32) + arrived[0, rows:].astype(F32), axis=0, keepdims=True)
    row = iota((8, width), 0)
    kept[rows:] = jnp.where(row == 0, both, 0.0)
    block = jnp.zeros((8, width), F32)
    for index, part in enumerate(split_bf16(both, 3)):
        block = jnp.where(row == index, part.astype(F32), block)
    for k in range(1, count):
        b = lax.rem(chip + k, count)
        sent[k - 1][:rows] = (mine[b, :rows].astype(F32) + arrived[b, :rows].astype(F32)).astype(BF16)
        sent[k - 1][rows:] = block.astype(BF16)


def finish(piece, kept, *refs):
    arrived, result = refs[:-1], refs[-1]
    rows = piece.shape[0]
    total = kept[:rows]
    squares = kept[rows:, :128]
    for part in arrived:
        total = total + part[:rows].astype(F32)
        squares = squares + part[rows:, :128].astype(F32)
    squares = jnp.broadcast_to(jnp.sum(squares, axis=0, keepdims=True), (rows, 128))
    scale = lax.rsqrt(jnp.transpose(squares) / INNER + EPS)
    for tile in range(piece.shape[1] // 128):
        span = slice(tile * 128, (tile + 1) * 128)
        result[:, span] = (piece[:, span].astype(F32) + scale * total[:, span]).astype(BF16)


def layer(piece, edge, weights):
    (
        prenorm,
        gate_weight,
        inner_weight,
        state_weight,
        step_weight,
        inner_taps,
        state_taps,
        step_bias,
        decay_rate,
        skip_scale,
        inner_gain,
        out_weight,
    ) = weights
    chip = lax.axis_index("chip").reshape(1)
    count = lax.axis_size("chip")
    members = lax.axis_size(SEQ)
    rows, block = piece.shape
    tall = 2 * rows
    width = inner_weight.shape[1]
    maps_width = state_weight.shape[1]
    heads = step_weight.shape[1]
    spread_rows = jnp.concatenate([edge, piece], axis=0)
    gain = prenorm.reshape(count, 1, block)
    steps_weight = step_weight.T

    def moved(step):
        return lax.ppermute(spread_rows, "chip", ring(count, step))

    far = moved(2)
    before = moved(1)
    after = moved(3)
    own = {0: spread_rows, 1: before, 2: far, 3: after}
    other = {k: lax.ppermute(part, "core", SWAP) for k, part in own.items()}
    near = [own[k] for k in NEAR] + [other[k] for k in NEAR]
    far = [own[k] for k in FAR] + [other[k] for k in FAR]
    high = 2 * spread_rows.shape[0]
    scaled, squares, *partial = local(
        enter_near,
        [*near, gain, steps_weight, state_weight, inner_weight],
        [
            ((len(NEAR), high, block), BF16),
            ((high, 128), F32),
            ((high, heads), F32),
            ((high, maps_width), F32),
            ((high, width), F32),
        ],
        weights=2,
        scratch=[
            *room(state_weight, len(NEAR), len(NEAR) * block),
            *room(inner_weight, len(NEAR), len(NEAR) * block),
        ],
    )
    scaled_far, scales, x, maps, steps, sums, sent = local(
        enter_far,
        [
            *far,
            squares,
            *partial,
            gain,
            steps_weight,
            inner_taps[:, None],
            state_taps[:, None],
            step_bias[None],
            decay_rate[None],
            state_weight,
            inner_weight,
        ],
        [
            ((len(FAR), high, block), BF16),
            ((tall, 128), F32),
            ((2, rows, width), BF16),
            ((2, rows, maps_width), BF16),
            ((2, rows, heads), F32),
            ((2, rows, heads), F32),
            ((tall, width + 128), BF16),
        ],
        weights=2,
        scratch=[
            *room(state_weight, len(FAR), len(FAR) * block),
            *room(inner_weight, len(FAR), len(FAR) * block),
        ],
    )
    arrived = lax.all_to_all(
        sent.reshape(members, tall // members, -1), SEQ, 0, 0, tiled=True
    )
    (gate,) = local(
        gate_project,
        [scaled, scaled_far, scales, gate_weight],
        [((tall, width), F32)],
        weights=1,
        scratch=room(gate_weight, count),
    )
    base, ahead = local(
        local_mixing,
        [x, maps, steps, sums, gate, skip_scale[None]],
        [((2, rows, width), F32), ((2, rows, width), F32)],
    )
    (back,) = local(scan_states, [arrived], [((members, tall // members, width), BF16)])
    back = lax.all_to_all(back, SEQ, 0, 0, tiled=True)
    entering = back.reshape(2, rows, width)
    mine, given = local(
        output_terms,
        [base, ahead, maps, entering, inner_gain[None], out_weight],
        [((count, rows + 8, block), BF16)] * 2,
        weights=1,
        scratch=room(out_weight, count),
    )
    taken = lax.ppermute(given, "core", SWAP)
    kept, *leaving = local(
        merge_cores,
        [chip, mine, taken],
        [((rows + 8, block), F32)] + [((rows + 8, block), BF16)] * (count - 1),
        scalars=1,
    )
    parts = [lax.ppermute(part, "chip", ring(count, k + 1)) for k, part in enumerate(leaving)]
    return local(finish, [piece, kept, *parts], [((rows, block), BF16)])[0]


def shards(
    tokens,
    prenorm_gain,
    gate_weight,
    inner_weight,
    state_weight,
    step_weight,
    inner_taps,
    state_taps,
    step_bias,
    decay_rate,
    skip_scale,
    inner_gain,
    out_weight,
):
    weights = (
        prenorm_gain[0],
        gate_weight[0],
        inner_weight[0],
        state_weight[0],
        step_weight[0],
        inner_taps[0],
        state_taps[0],
        step_bias[0],
        decay_rate[0],
        skip_scale[0],
        inner_gain[0],
        out_weight[0],
    )
    sections = lax.axis_size("pipe")
    section = lax.axis_index("pipe")
    core = lax.axis_index("core")
    width = tokens.shape[2]
    members = lax.axis_size(SEQ)
    edges = lax.ppermute(tokens[:, -EDGE:], SEQ, [(s, s + 1) for s in range(members - 1)])
    rows = jnp.concatenate([edges, tokens], axis=1)
    mine = jnp.where(core == 0, rows[0], rows[1])
    given = lax.ppermute(jnp.where(core == 0, rows[1], rows[0]), "core", SWAP)

    def joined(left, right):
        return jnp.where(
            core == 0, jnp.concatenate([left, right], 1), jnp.concatenate([right, left], 1)
        )

    joint = joined(mine, given)
    piece, edge = joint[EDGE:], joint[:EDGE]
    kept = None
    for turn in range(sections):
        own = layer(piece, edge, weights)
        kept = own if turn == 0 else jnp.where(section == turn, own, kept)
        if turn + 1 < sections:
            piece = lax.ppermute(own, "pipe", [(s, s + 1) for s in range(sections - 1)])
            edge = lax.ppermute(
                own[-EDGE:],
                ("pipe", *SEQ),
                [
                    (p * members + s, (p + 1) * members + s + 1)
                    for p in range(sections - 1)
                    for s in range(members - 1)
                ],
            )
    left, right = kept[:, :width], kept[:, width:]
    held = jnp.where(core == 0, left, right)
    given = lax.ppermute(jnp.where(core == 0, right, left), "core", SWAP)
    return jnp.where(core == 0, jnp.stack([held, given]), jnp.stack([given, held]))[None]


def solution(mesh):
    torus = Mesh(
        mesh.devices.reshape(mesh.shape["pipe"], mesh.shape["tensor"] // 2, 2, 8, 2),
        ("pipe", "chip", "core", "seq_0", "seq_1"),
    )
    return jax.shard_map(
        shards,
        mesh=torus,
        in_specs=(
            P(None, SEQ, TENSOR),
            P("pipe", None),
            P("pipe", None, TENSOR),
            P("pipe", None, TENSOR),
            P("pipe", None, None),
            P("pipe", None, TENSOR),
            P("pipe", None, TENSOR),
            P("pipe", None, None),
            P("pipe", TENSOR),
            P("pipe", TENSOR),
            P("pipe", TENSOR),
            P("pipe", TENSOR),
            P("pipe", TENSOR, None),
        ),
        out_specs=P("pipe", None, SEQ, TENSOR),
        check_vma=False,
    )
```

```python
import jax
import jax.numpy as jnp
from jax import lax
from jax.experimental import pallas as pl
from jax.experimental.pallas import tpu as pltpu
from jax.sharding import Mesh
from jax.sharding import PartitionSpec as P

INNER = 5120
EPS = 1e-05
EDGE = 8
NEAR = (0,)
FAR = (2, 1, 3)
SEQ = ("seq_0", "seq_1")
CROSS = ("seq_1", "seq_0")
TENSOR = ("chip", "core")
SWAP = [(0, 1), (1, 0)]
F32 = jnp.float32
BF16 = jnp.bfloat16
VMEM = pl.BlockSpec(memory_space=pltpu.VMEM)
SMEM = pl.BlockSpec(memory_space=pltpu.SMEM)
HBM = pl.BlockSpec(memory_space=pltpu.MemorySpace.HBM)


def ring(size, steps):
    return [(source, (source + steps) % size) for source in range(size)]


def split_bf16(value, count):
    parts = []
    for _ in range(count):
        part = value.astype(BF16)
        parts.append(part)
        value = value - part.astype(F32)
    return parts


def local(body, args, outs, scalars=0, weights=0, scratch=(), mib=16, flops=1 << 28):
    first = len(args) - weights
    args = [
        pltpu.with_memory_space_constraint(arg, pltpu.MemorySpace.HBM) if index >= first else arg
        for index, arg in enumerate(args)
    ]
    return pl.pallas_call(
        body,
        out_shape=[jax.ShapeDtypeStruct(shape, kind) for shape, kind in outs],
        in_specs=[SMEM] * scalars + [VMEM] * (len(args) - scalars - weights) + [HBM] * weights,
        out_specs=[VMEM] * len(outs),
        cost_estimate=pl.CostEstimate(flops=flops, transcendentals=0, bytes_accessed=1 << 22),
        scratch_shapes=list(scratch),
        compiler_params=pltpu.CompilerParams(vmem_limit_bytes=mib << 20),
    )(*args)


def fetch(source, target, semaphores, blocks=None):
    parts = semaphores.shape[0]
    size = target.shape[0] // parts
    copies = [
        pltpu.make_async_copy(
            source.at[pl.ds((part if blocks is None else blocks[part]) * size, size)],
            target.at[pl.ds(part * size, size)],
            semaphores.at[part],
        )
        for part in range(parts)
    ]
    for copy in copies:
        copy.start()
    return copies


def blocks_of(steps):
    chip, count = lax.axis_index("chip"), 4
    return [lax.rem(chip - step + count, count) for step in steps]


def fetch_columns(source, target, semaphores):
    parts = semaphores.shape[0]
    size = target.shape[1] // parts
    copies = [
        pltpu.make_async_copy(
            source.at[:, pl.ds(part * size, size)],
            target.at[:, pl.ds(part * size, size)],
            semaphores.at[part],
        )
        for part in range(parts)
    ]
    for copy in copies:
        copy.start()
    return copies


def room(weight, parts, rows=None):
    shape = (rows or weight.shape[0], weight.shape[1])
    return [pltpu.VMEM(shape, weight.dtype), pltpu.SemaphoreType.DMA((parts,))]


def dot(a, b, dims=((1,), (0,))):
    return lax.dot_general(a, b, (dims, ((), ())), preferred_element_type=F32)


def sigmoid(value):
    return 1.0 / (1.0 + jnp.exp(-value))


def iota(shape, dim):
    return lax.broadcasted_iota(jnp.int32, shape, dim)


def spread(heads, width, copies=1):
    size = width // heads
    lane, head = iota((heads * copies, width), 1), iota((heads * copies, width), 0) % heads
    return jnp.where((lane >= head * size) & (lane < (head + 1) * size), 1.0, 0.0).astype(BF16)


def over_channels(value, width):
    parts = [part.astype(F32) for part in split_bf16(value, 3)]
    return dot(jnp.concatenate(parts, 1).astype(BF16), spread(value.shape[1], width, 3))


def convolve(rim, values, taps):
    width = taps.shape[0] - 1
    length = values.shape[0]
    padded = jnp.concatenate([rim, values], axis=0).astype(F32)
    lead = rim.shape[0] - width + 1
    total = taps[width]
    for index in range(width):
        total = total + taps[index] * padded[lead + index : lead + index + length]
    return (total * sigmoid(total)).astype(BF16)


def place(piece, gain, scaled, side, edge):
    rows = piece.shape[0] - edge
    value = piece[...].astype(F32)
    square = value * value
    squares = 0.0
    for tile in range(piece.shape[1] // 128):
        squares = squares + square[:, tile * 128 : (tile + 1) * 128]
    value = value * gain
    scaled[side * rows : (side + 1) * rows, :] = value[edge:].astype(BF16)
    return squares, value[:edge]


def columns(array, b, width):
    return array[:, pl.ds(pl.multiple_of(b * width, width), width)]


def multiply(scaled, part, step_w, state_w, inner_w, copies):
    block = scaled.shape[1]
    span = slice(part * block, (part + 1) * block)
    value = scaled[...]
    step = dot(value, step_w, ((1,), (1,)))
    copies[0][part].wait()
    state = dot(value, state_w[span, :])
    copies[1][part].wait()
    return step, state, dot(value, inner_w[span, :])


def enter_near(*refs):
    count = len(NEAR)
    sides = refs[:count], refs[count : 2 * count]
    gain, step_w, state_hbm, inner_hbm = refs[2 * count :][:4]
    scaled, squares, step, state, inner = refs[2 * count + 4 :][:5]
    state_w, state_sems, inner_w, inner_sems = refs[2 * count + 9 :]
    blocks = blocks_of(NEAR)
    copies = fetch(state_hbm, state_w, state_sems, blocks), fetch(
        inner_hbm, inner_w, inner_sems, blocks
    )
    edge = EDGE
    rows = sides[0][0].shape[0] - edge
    width = sides[0][0].shape[1]
    sums = [0.0, 0.0]
    totals = [0.0, 0.0, 0.0]
    for k, b in enumerate(blocks):
        tails = []
        for side in range(2):
            part, tail = place(sides[side][k], gain[b], scaled.at[k], side, edge)
            sums[side] = sums[side] + part
            tails.append(tail)
        scaled[k, 2 * rows :, :] = jnp.concatenate(tails).astype(BF16)
        parts = multiply(scaled.at[k], k, columns(step_w, b, width), state_w, inner_w, copies)
        totals = [total + part for total, part in zip(totals, parts)]
    for side in range(2):
        squares[side * rows : (side + 1) * rows, :] = sums[side][edge:]
        squares[2 * rows + side * edge : 2 * rows + (side + 1) * edge, :] = sums[side][:edge]
    step[...], state[...], inner[...] = totals


def enter_far(*refs):
    count = len(FAR)
    sides = refs[:count], refs[count : 2 * count]
    squares_in, step_in, state_in, inner_in = refs[2 * count :][:4]
    refs = refs[2 * count + 4 :]
    gain, step_w, inner_taps, state_taps, bias, rate, state_hbm, inner_hbm = refs[:8]
    scaled, scales, x, maps, steps, sums, sent = refs[8:15]
    state_w, state_sems, inner_w, inner_sems = refs[15:]
    blocks = blocks_of(FAR)
    copies = fetch(state_hbm, state_w, state_sems, blocks), fetch(
        inner_hbm, inner_w, inner_sems, blocks
    )
    edge = EDGE
    rows, width = x.shape[1:]
    block = sides[0][0].shape[1]
    heads = bias.shape[1]
    n = maps.shape[2] // 2
    found = [0.0, 0.0]
    for k, b in enumerate(blocks):
        tails = []
        for side in range(2):
            part, tail = place(sides[side][k], gain[b], scaled.at[k], side, edge)
            found[side] = found[side] + part
            tails.append(tail)
        scaled[k, 2 * rows :, :] = jnp.concatenate(tails).astype(BF16)
    found = jnp.concatenate([found[0][edge:], found[1][edge:], found[0][:edge], found[1][:edge]])
    squares = jnp.sum(squares_in[...] + found, axis=1, keepdims=True)
    scale = lax.rsqrt(squares / (len(NEAR + FAR) * block) + EPS)
    scales[...] = jnp.broadcast_to(scale[: 2 * rows], scales.shape)
    totals = [step_in[...], state_in[...], inner_in[...]]
    for k, b in enumerate(blocks):
        parts = multiply(scaled.at[k], k, columns(step_w, b, block), state_w, inner_w, copies)
        totals = [total + part for total, part in zip(totals, parts)]
    step, state, inner = totals
    raw = (step * scale)[: 2 * rows] + bias[...]
    step_all = jnp.maximum(raw, 0.0) + jnp.log1p(jnp.exp(-jnp.abs(raw)))
    state = (state * scale).astype(BF16).astype(F32)
    inner = (inner * scale).astype(BF16).astype(F32)
    lower = (iota((rows, rows), 0) >= iota((rows, rows), 1)).astype(BF16)
    for m in range(2):
        span = slice(m * rows, (m + 1) * rows)
        ends = slice(2 * rows + m * edge, 2 * rows + (m + 1) * edge)
        sm = convolve(state[ends], state[span], state_taps)
        xm = convolve(inner[ends], inner[span], inner_taps)
        x[m] = xm
        maps[m] = sm
        step = step_all[span]
        total = -sum(dot(lower, part) for part in split_bf16(step * rate[...], 3))
        last = total[rows - 1 :]
        steps[m] = step
        sums[m] = total
        weighting = over_channels(jnp.exp(last - total) * step, width)
        weighted = (xm.astype(F32) * weighting).astype(BF16)
        sent[span, :width] = dot(sm[:, :n], weighted, ((0,), (0,))).astype(BF16)
        high, low = split_bf16(jnp.exp(last), 2)
        row = iota((rows, heads), 0) % 16
        ends = jnp.where(row == 0, high.astype(F32), low.astype(F32))
        ends = jnp.concatenate([ends, jnp.zeros((rows, sent.shape[1] - width - heads), F32)], 1)
        sent[span, width:] = ends.astype(BF16)


def gate_project(near, far, scales, gate_hbm, gate, gate_w, gate_sems):
    copies = fetch(gate_hbm, gate_w, gate_sems, blocks_of(NEAR + FAR))
    rows, width = gate.shape
    block = far.shape[2]
    total = 0.0
    for part in range(len(NEAR + FAR)):
        scaled = near[part, :rows] if part < len(NEAR) else far[part - len(NEAR), :rows]
        copies[part].wait()
        total = total + dot(scaled, gate_w[part * block : (part + 1) * block, :])
    for tile in range(width // 128):
        span = slice(tile * 128, (tile + 1) * 128)
        value = (total[:, span] * scales[...]).astype(BF16).astype(F32)
        gate[:, span] = value * sigmoid(value)


def local_mixing(x, maps, steps, sums, gate, skip, base, ahead):
    micros, rows, width = x.shape
    heads = skip.shape[1]
    size = width // heads
    pair = 128 // size
    n = maps.shape[2] // 2
    skips = over_channels(jnp.broadcast_to(skip[...], (8, heads)), width)[:1]
    later = iota((rows, rows), 0) >= iota((rows, rows), 1)
    lane = iota((rows, pair * size), 1)
    for m in range(micros):
        maps_m, sums_m, steps_m = maps[m], sums[m], steps[m]
        scores = dot(maps_m[:, n:], maps_m[:, :n], ((1,), (1,)))
        fill = jnp.zeros((rows, 128 - heads), F32)
        sums_t = jnp.transpose(jnp.concatenate([sums_m, fill], 1))
        steps_t = jnp.transpose(jnp.concatenate([steps_m, fill], 1))
        for g in range(heads // pair):
            span = slice(g * pair * size, (g + 1) * pair * size)
            xg = x[m, :, span]
            left, right = [], []
            for j in range(pair):
                h = g * pair + j
                gap = sums_m[:, h : h + 1] - sums_t[h : h + 1, :]
                decay = jnp.exp(jnp.where(later, gap, -jnp.inf))
                left.append((scores * decay * steps_t[h : h + 1, :]).astype(BF16))
                right.append(
                    jnp.where((lane >= j * size) & (lane < (j + 1) * size), xg, jnp.zeros_like(xg))
                )
            inside = dot(jnp.concatenate(left, 1), jnp.concatenate(right, 0))
            silu = gate[m * rows : (m + 1) * rows, span]
            base[m, :, span] = (inside + skips[:, span] * xg.astype(F32)) * silu
        ahead[m] = over_channels(jnp.exp(sums_m), width) * gate[m * rows : (m + 1) * rows]


def scan_states(arrived, back, heads=10):
    members, rows, width = back.shape
    picks = spread(128, 128 * (width // heads))[:, :width]
    ends = arrived[:, :, width:].reshape(members * rows, arrived.shape[2] - width)
    factors = dot(ends, picks)
    running = jnp.zeros((rows, width), F32)
    for position in range(members):
        s = position % 2 * (members // 2) + position // 2
        back[s] = running.astype(BF16)
        factor = factors[s * rows : s * rows + 1] + factors[s * rows + 1 : s * rows + 2]
        running = running * factor + arrived[s, :, :width].astype(F32)


def squares_rows(squares):
    rows = squares.shape[0]
    lane = iota((rows, 128), 1)
    block = jnp.zeros((rows, 128), F32)
    for index, part in enumerate(split_bf16(squares, 3)):
        block = jnp.where(lane == index, part.astype(F32), block)
    return jnp.transpose(block)[:8]


def output_terms(base, ahead, maps, entering, gain, out_hbm, mine, given, out_w, out_sems):
    n = maps.shape[2] // 2
    count, _, width = mine.shape
    copies = fetch_columns(out_hbm, out_w, out_sems)
    rows = base.shape[1]
    scaled = []
    for m, term in enumerate((mine, given)):
        across = dot(maps[m, :, n:], entering[m])
        gated = base[m] + across * ahead[m]
        squares = jnp.sum(gated * gated, axis=1, keepdims=True)
        scaled.append((gated * gain[...]).astype(BF16))
        block = squares_rows(squares)
        block = jnp.concatenate([block, jnp.zeros((8, width - 128), F32)], 1).astype(term.dtype)
        for b in range(count):
            term[b, rows:] = block
    scaled = jnp.concatenate(scaled)
    for b in range(count):
        copies[b].wait()
        value = dot(scaled, out_w[:, b * width : (b + 1) * width])
        mine[b, :rows] = value[:rows].astype(mine.dtype)
        given[b, :rows] = value[rows:].astype(given.dtype)


def merge_cores(chip_ref, mine, arrived, kept, *sent):
    count, tall, width = mine.shape
    rows = tall - 8
    chip = chip_ref[0]
    kept[:rows] = mine[chip, :rows].astype(F32) + arrived[chip, :rows].astype(F32)
    both = jnp.sum(mine[0, rows:].astype(F32) + arrived[0, rows:].astype(F32), axis=0, keepdims=True)
    row = iota((8, width), 0)
    kept[rows:] = jnp.where(row == 0, both, 0.0)
    block = jnp.zeros((8, width), F32)
    for index, part in enumerate(split_bf16(both, 3)):
        block = jnp.where(row == index, part.astype(F32), block)
    for k in range(1, count):
        b = lax.rem(chip + k, count)
        sent[k - 1][:rows] = (mine[b, :rows].astype(F32) + arrived[b, :rows].astype(F32)).astype(BF16)
        sent[k - 1][rows:] = block.astype(BF16)


def finish(piece, kept, *refs):
    arrived, result = refs[:-1], refs[-1]
    rows = piece.shape[0]
    total = kept[:rows]
    squares = kept[rows:, :128]
    for part in arrived:
        total = total + part[:rows].astype(F32)
        squares = squares + part[rows:, :128].astype(F32)
    squares = jnp.broadcast_to(jnp.sum(squares, axis=0, keepdims=True), (rows, 128))
    scale = lax.rsqrt(jnp.transpose(squares) / INNER + EPS)
    for tile in range(piece.shape[1] // 128):
        span = slice(tile * 128, (tile + 1) * 128)
        result[:, span] = (piece[:, span].astype(F32) + scale * total[:, span]).astype(BF16)


def layer(piece, edge, weights):
    (
        prenorm,
        gate_weight,
        inner_weight,
        state_weight,
        step_weight,
        inner_taps,
        state_taps,
        step_bias,
        decay_rate,
        skip_scale,
        inner_gain,
        out_weight,
    ) = weights
    chip = lax.axis_index("chip").reshape(1)
    count = lax.axis_size("chip")
    members = lax.axis_size(SEQ)
    rows, block = piece.shape
    tall = 2 * rows
    width = inner_weight.shape[1]
    maps_width = state_weight.shape[1]
    heads = step_weight.shape[1]
    spread_rows = jnp.concatenate([edge, piece], axis=0)
    gain = prenorm.reshape(count, 1, block)
    steps_weight = step_weight.T

    def moved(step):
        return lax.ppermute(spread_rows, "chip", ring(count, step))

    far = moved(2)
    before = moved(1)
    after = moved(3)
    own = {0: spread_rows, 1: before, 2: far, 3: after}
    other = {k: lax.ppermute(part, "core", SWAP) for k, part in own.items()}
    near = [own[k] for k in NEAR] + [other[k] for k in NEAR]
    far = [own[k] for k in FAR] + [other[k] for k in FAR]
    high = 2 * spread_rows.shape[0]
    scaled, squares, *partial = local(
        enter_near,
        [*near, gain, steps_weight, state_weight, inner_weight],
        [
            ((len(NEAR), high, block), BF16),
            ((high, 128), F32),
            ((high, heads), F32),
            ((high, maps_width), F32),
            ((high, width), F32),
        ],
        weights=2,
        scratch=[
            *room(state_weight, len(NEAR), len(NEAR) * block),
            *room(inner_weight, len(NEAR), len(NEAR) * block),
        ],
    )
    scaled_far, scales, x, maps, steps, sums, sent = local(
        enter_far,
        [
            *far,
            squares,
            *partial,
            gain,
            steps_weight,
            inner_taps[:, None],
            state_taps[:, None],
            step_bias[None],
            decay_rate[None],
            state_weight,
            inner_weight,
        ],
        [
            ((len(FAR), high, block), BF16),
            ((tall, 128), F32),
            ((2, rows, width), BF16),
            ((2, rows, maps_width), BF16),
            ((2, rows, heads), F32),
            ((2, rows, heads), F32),
            ((tall, width + 128), BF16),
        ],
        weights=2,
        scratch=[
            *room(state_weight, len(FAR), len(FAR) * block),
            *room(inner_weight, len(FAR), len(FAR) * block),
        ],
    )
    arrived = lax.all_to_all(sent.reshape(members, tall // members, -1), CROSS, 0, 0, tiled=True)
    (gate,) = local(
        gate_project,
        [scaled, scaled_far, scales, gate_weight],
        [((tall, width), F32)],
        weights=1,
        scratch=room(gate_weight, count),
    )
    base, ahead = local(
        local_mixing,
        [x, maps, steps, sums, gate, skip_scale[None]],
        [((2, rows, width), F32), ((2, rows, width), F32)],
    )
    (back,) = local(scan_states, [arrived], [((members, tall // members, width), BF16)])
    back = lax.all_to_all(back, CROSS, 0, 0, tiled=True)
    entering = back.reshape(2, rows, width)
    mine, given = local(
        output_terms,
        [base, ahead, maps, entering, inner_gain[None], out_weight],
        [((count, rows + 8, block), BF16)] * 2,
        weights=1,
        scratch=room(out_weight, count),
    )
    taken = lax.ppermute(given, "core", SWAP)
    kept, *leaving = local(
        merge_cores,
        [chip, mine, taken],
        [((rows + 8, block), F32)] + [((rows + 8, block), BF16)] * (count - 1),
        scalars=1,
    )
    parts = [lax.ppermute(part, "chip", ring(count, k + 1)) for k, part in enumerate(leaving)]
    return local(finish, [piece, kept, *parts], [((rows, block), BF16)])[0]


def shards(
    tokens,
    prenorm_gain,
    gate_weight,
    inner_weight,
    state_weight,
    step_weight,
    inner_taps,
    state_taps,
    step_bias,
    decay_rate,
    skip_scale,
    inner_gain,
    out_weight,
):
    weights = (
        prenorm_gain[0],
        gate_weight[0],
        inner_weight[0],
        state_weight[0],
        step_weight[0],
        inner_taps[0],
        state_taps[0],
        step_bias[0],
        decay_rate[0],
        skip_scale[0],
        inner_gain[0],
        out_weight[0],
    )
    sections = lax.axis_size("pipe")
    section = lax.axis_index("pipe")
    core = lax.axis_index("core")
    width = tokens.shape[2]
    members = lax.axis_size(SEQ)
    edges = lax.ppermute(tokens[:, -EDGE:], SEQ, [(s, s + 1) for s in range(members - 1)])
    rows = jnp.concatenate([edges, tokens], axis=1)
    mine = jnp.where(core == 0, rows[0], rows[1])
    given = lax.ppermute(jnp.where(core == 0, rows[1], rows[0]), "core", SWAP)

    def joined(left, right):
        return jnp.where(
            core == 0, jnp.concatenate([left, right], 1), jnp.concatenate([right, left], 1)
        )

    joint = joined(mine, given)
    piece, edge = joint[EDGE:], joint[:EDGE]
    kept = None
    for turn in range(sections):
        own = layer(piece, edge, weights)
        kept = own if turn == 0 else jnp.where(section == turn, own, kept)
        if turn + 1 < sections:
            piece = lax.ppermute(own, "pipe", [(s, s + 1) for s in range(sections - 1)])
            edge = lax.ppermute(
                own[-EDGE:],
                ("pipe", *SEQ),
                [
                    (p * members + s, (p + 1) * members + s + 1)
                    for p in range(sections - 1)
                    for s in range(members - 1)
                ],
            )
    left, right = kept[:, :width], kept[:, width:]
    held = jnp.where(core == 0, left, right)
    given = lax.ppermute(jnp.where(core == 0, right, left), "core", SWAP)
    return jnp.where(core == 0, jnp.stack([held, given]), jnp.stack([given, held]))[None]


def solution(mesh):
    torus = Mesh(
        mesh.devices.reshape(mesh.shape["pipe"], mesh.shape["tensor"] // 2, 2, 8, 2),
        ("pipe", "chip", "core", "seq_0", "seq_1"),
    )
    return jax.shard_map(
        shards,
        mesh=torus,
        in_specs=(
            P(None, SEQ, TENSOR),
            P("pipe", None),
            P("pipe", None, TENSOR),
            P("pipe", None, TENSOR),
            P("pipe", None, None),
            P("pipe", None, TENSOR),
            P("pipe", None, TENSOR),
            P("pipe", None, None),
            P("pipe", TENSOR),
            P("pipe", TENSOR),
            P("pipe", TENSOR),
            P("pipe", TENSOR),
            P("pipe", TENSOR, None),
        ),
        out_specs=P("pipe", None, SEQ, TENSOR),
        check_vma=False,
    )
```

```python
import jax
import jax.numpy as jnp
from jax import lax
from jax.experimental import pallas as pl
from jax.experimental.pallas import tpu as pltpu
from jax.sharding import Mesh
from jax.sharding import PartitionSpec as P

INNER = 5120
EPS = 1e-05
EDGE = 8
NEAR = (0,)
FAR = (2, 1, 3)
SEQ = ("seq_0", "seq_1")
CROSS = ("seq_1", "seq_0")
TENSOR = ("chip", "core")
SWAP = [(0, 1), (1, 0)]
F32 = jnp.float32
BF16 = jnp.bfloat16
VMEM = pl.BlockSpec(memory_space=pltpu.VMEM)
SMEM = pl.BlockSpec(memory_space=pltpu.SMEM)
HBM = pl.BlockSpec(memory_space=pltpu.MemorySpace.HBM)


def ring(size, steps):
    return [(source, (source + steps) % size) for source in range(size)]


def split_bf16(value, count):
    parts = []
    for _ in range(count):
        part = value.astype(BF16)
        parts.append(part)
        value = value - part.astype(F32)
    return parts


def local(body, args, outs, scalars=0, weights=0, scratch=(), mib=16, flops=1 << 28):
    first = len(args) - weights
    args = [
        pltpu.with_memory_space_constraint(arg, pltpu.MemorySpace.HBM) if index >= first else arg
        for index, arg in enumerate(args)
    ]
    return pl.pallas_call(
        body,
        out_shape=[jax.ShapeDtypeStruct(shape, kind) for shape, kind in outs],
        in_specs=[SMEM] * scalars + [VMEM] * (len(args) - scalars - weights) + [HBM] * weights,
        out_specs=[VMEM] * len(outs),
        cost_estimate=pl.CostEstimate(flops=flops, transcendentals=0, bytes_accessed=1 << 22),
        scratch_shapes=list(scratch),
        compiler_params=pltpu.CompilerParams(vmem_limit_bytes=mib << 20),
    )(*args)


def fetch(source, target, semaphores, blocks=None):
    parts = semaphores.shape[0]
    size = target.shape[0] // parts
    copies = [
        pltpu.make_async_copy(
            source.at[pl.ds((part if blocks is None else blocks[part]) * size, size)],
            target.at[pl.ds(part * size, size)],
            semaphores.at[part],
        )
        for part in range(parts)
    ]
    for copy in copies:
        copy.start()
    return copies


def blocks_of(steps):
    chip, count = lax.axis_index("chip"), 4
    return [lax.rem(chip - step + count, count) for step in steps]


def fetch_columns(source, target, semaphores):
    parts = semaphores.shape[0]
    size = target.shape[1] // parts
    copies = [
        pltpu.make_async_copy(
            source.at[:, pl.ds(part * size, size)],
            target.at[:, pl.ds(part * size, size)],
            semaphores.at[part],
        )
        for part in range(parts)
    ]
    for copy in copies:
        copy.start()
    return copies


def room(weight, parts, rows=None):
    shape = (rows or weight.shape[0], weight.shape[1])
    return [pltpu.VMEM(shape, weight.dtype), pltpu.SemaphoreType.DMA((parts,))]


def dot(a, b, dims=((1,), (0,))):
    return lax.dot_general(a, b, (dims, ((), ())), preferred_element_type=F32)


def sigmoid(value):
    return 1.0 / (1.0 + jnp.exp(-value))


def iota(shape, dim):
    return lax.broadcasted_iota(jnp.int32, shape, dim)


def spread(heads, width, copies=1):
    size = width // heads
    lane, head = iota((heads * copies, width), 1), iota((heads * copies, width), 0) % heads
    return jnp.where((lane >= head * size) & (lane < (head + 1) * size), 1.0, 0.0).astype(BF16)


def over_channels(value, width):
    parts = [part.astype(F32) for part in split_bf16(value, 3)]
    return dot(jnp.concatenate(parts, 1).astype(BF16), spread(value.shape[1], width, 3))


def convolve(rim, values, taps):
    width = taps.shape[0] - 1
    length = values.shape[0]
    padded = jnp.concatenate([rim, values], axis=0).astype(F32)
    lead = rim.shape[0] - width + 1
    total = taps[width]
    for index in range(width):
        total = total + taps[index] * padded[lead + index : lead + index + length]
    return (total * sigmoid(total)).astype(BF16)


def place(piece, gain, scaled, side, edge):
    rows = piece.shape[0] - edge
    value = piece[...].astype(F32)
    square = value * value
    squares = 0.0
    for tile in range(piece.shape[1] // 128):
        squares = squares + square[:, tile * 128 : (tile + 1) * 128]
    value = value * gain
    scaled[side * rows : (side + 1) * rows, :] = value[edge:].astype(BF16)
    return squares, value[:edge]


def columns(array, b, width):
    return array[:, pl.ds(pl.multiple_of(b * width, width), width)]


def multiply(scaled, part, step_w, state_w, inner_w, copies):
    block = scaled.shape[1]
    span = slice(part * block, (part + 1) * block)
    value = scaled[...]
    step = dot(value, step_w, ((1,), (1,)))
    if copies is not None:
        copies[0][part].wait()
    state = dot(value, state_w[span, :])
    if copies is not None:
        copies[1][part].wait()
    return step, state, dot(value, inner_w[span, :])


def enter_near(*refs):
    count = len(NEAR)
    sides = refs[:count], refs[count : 2 * count]
    gain, step_w, state_hbm, inner_hbm = refs[2 * count :][:4]
    scaled, squares, step, state, inner, state_rest, inner_rest = refs[2 * count + 4 :][:7]
    state_w, state_sems, inner_w, inner_sems, state_rest_sems, inner_rest_sems = refs[
        2 * count + 11 :
    ]
    blocks = blocks_of(NEAR)
    copies = fetch(state_hbm, state_w, state_sems, blocks), fetch(
        inner_hbm, inner_w, inner_sems, blocks
    )
    rest = fetch(state_hbm, state_rest, state_rest_sems, blocks_of(FAR))
    rest += fetch(inner_hbm, inner_rest, inner_rest_sems, blocks_of(FAR))
    edge = EDGE
    rows = sides[0][0].shape[0] - edge
    width = sides[0][0].shape[1]
    sums = [0.0, 0.0]
    totals = [0.0, 0.0, 0.0]
    for k, b in enumerate(blocks):
        tails = []
        for side in range(2):
            part, tail = place(sides[side][k], gain[b], scaled.at[k], side, edge)
            sums[side] = sums[side] + part
            tails.append(tail)
        scaled[k, 2 * rows :, :] = jnp.concatenate(tails).astype(BF16)
        parts = multiply(scaled.at[k], k, columns(step_w, b, width), state_w, inner_w, copies)
        totals = [total + part for total, part in zip(totals, parts)]
    for side in range(2):
        squares[side * rows : (side + 1) * rows, :] = sums[side][edge:]
        squares[2 * rows + side * edge : 2 * rows + (side + 1) * edge, :] = sums[side][:edge]
    step[...], state[...], inner[...] = totals
    for copy in rest:
        copy.wait()


def enter_far(*refs):
    count = len(FAR)
    sides = refs[:count], refs[count : 2 * count]
    squares_in, step_in, state_in, inner_in = refs[2 * count :][:4]
    refs = refs[2 * count + 4 :]
    gain, step_w, inner_taps, state_taps, bias, rate, state_w, inner_w = refs[:8]
    scaled, scales, x, maps, steps, sums, sent = refs[8:]
    blocks = blocks_of(FAR)
    edge = EDGE
    rows, width = x.shape[1:]
    block = sides[0][0].shape[1]
    heads = bias.shape[1]
    n = maps.shape[2] // 2
    found = [0.0, 0.0]
    for k, b in enumerate(blocks):
        tails = []
        for side in range(2):
            part, tail = place(sides[side][k], gain[b], scaled.at[k], side, edge)
            found[side] = found[side] + part
            tails.append(tail)
        scaled[k, 2 * rows :, :] = jnp.concatenate(tails).astype(BF16)
    found = jnp.concatenate([found[0][edge:], found[1][edge:], found[0][:edge], found[1][:edge]])
    squares = jnp.sum(squares_in[...] + found, axis=1, keepdims=True)
    scale = lax.rsqrt(squares / (len(NEAR + FAR) * block) + EPS)
    scales[...] = jnp.broadcast_to(scale[: 2 * rows], scales.shape)
    totals = [step_in[...], state_in[...], inner_in[...]]
    for k, b in enumerate(blocks):
        parts = multiply(scaled.at[k], k, columns(step_w, b, block), state_w, inner_w, None)
        totals = [total + part for total, part in zip(totals, parts)]
    step, state, inner = totals
    raw = (step * scale)[: 2 * rows] + bias[...]
    step_all = jnp.maximum(raw, 0.0) + jnp.log1p(jnp.exp(-jnp.abs(raw)))
    state = (state * scale).astype(BF16).astype(F32)
    inner = (inner * scale).astype(BF16).astype(F32)
    lower = (iota((rows, rows), 0) >= iota((rows, rows), 1)).astype(BF16)
    for m in range(2):
        span = slice(m * rows, (m + 1) * rows)
        ends = slice(2 * rows + m * edge, 2 * rows + (m + 1) * edge)
        sm = convolve(state[ends], state[span], state_taps)
        xm = convolve(inner[ends], inner[span], inner_taps)
        x[m] = xm
        maps[m] = sm
        step = step_all[span]
        total = -sum(dot(lower, part) for part in split_bf16(step * rate[...], 3))
        last = total[rows - 1 :]
        steps[m] = step
        sums[m] = total
        weighting = over_channels(jnp.exp(last - total) * step, width)
        weighted = (xm.astype(F32) * weighting).astype(BF16)
        sent[span, :width] = dot(sm[:, :n], weighted, ((0,), (0,))).astype(BF16)
        high, low = split_bf16(jnp.exp(last), 2)
        row = iota((rows, heads), 0) % 16
        ends = jnp.where(row == 0, high.astype(F32), low.astype(F32))
        ends = jnp.concatenate([ends, jnp.zeros((rows, sent.shape[1] - width - heads), F32)], 1)
        sent[span, width:] = ends.astype(BF16)


def gate_project(near, far, scales, gate_hbm, gate, gate_w, gate_sems):
    copies = fetch(gate_hbm, gate_w, gate_sems, blocks_of(NEAR + FAR))
    rows, width = gate.shape
    block = far.shape[2]
    total = 0.0
    for part in range(len(NEAR + FAR)):
        scaled = near[part, :rows] if part < len(NEAR) else far[part - len(NEAR), :rows]
        copies[part].wait()
        total = total + dot(scaled, gate_w[part * block : (part + 1) * block, :])
    for tile in range(width // 128):
        span = slice(tile * 128, (tile + 1) * 128)
        value = (total[:, span] * scales[...]).astype(BF16).astype(F32)
        gate[:, span] = value * sigmoid(value)


def local_mixing(x, maps, steps, sums, gate, skip, base, ahead):
    micros, rows, width = x.shape
    heads = skip.shape[1]
    size = width // heads
    pair = 128 // size
    n = maps.shape[2] // 2
    skips = over_channels(jnp.broadcast_to(skip[...], (8, heads)), width)[:1]
    later = iota((rows, rows), 0) >= iota((rows, rows), 1)
    lane = iota((rows, pair * size), 1)
    for m in range(micros):
        maps_m, sums_m, steps_m = maps[m], sums[m], steps[m]
        scores = dot(maps_m[:, n:], maps_m[:, :n], ((1,), (1,)))
        fill = jnp.zeros((rows, 128 - heads), F32)
        sums_t = jnp.transpose(jnp.concatenate([sums_m, fill], 1))
        steps_t = jnp.transpose(jnp.concatenate([steps_m, fill], 1))
        for g in range(heads // pair):
            span = slice(g * pair * size, (g + 1) * pair * size)
            xg = x[m, :, span]
            left, right = [], []
            for j in range(pair):
                h = g * pair + j
                gap = sums_m[:, h : h + 1] - sums_t[h : h + 1, :]
                decay = jnp.exp(jnp.where(later, gap, -jnp.inf))
                left.append((scores * decay * steps_t[h : h + 1, :]).astype(BF16))
                right.append(
                    jnp.where((lane >= j * size) & (lane < (j + 1) * size), xg, jnp.zeros_like(xg))
                )
            inside = dot(jnp.concatenate(left, 1), jnp.concatenate(right, 0))
            silu = gate[m * rows : (m + 1) * rows, span]
            base[m, :, span] = (inside + skips[:, span] * xg.astype(F32)) * silu
        ahead[m] = over_channels(jnp.exp(sums_m), width) * gate[m * rows : (m + 1) * rows]


def scan_states(arrived, back, heads=10):
    members, rows, width = back.shape
    picks = spread(128, 128 * (width // heads))[:, :width]
    ends = arrived[:, :, width:].reshape(members * rows, arrived.shape[2] - width)
    factors = dot(ends, picks)
    running = jnp.zeros((rows, width), F32)
    for position in range(members):
        s = position % 2 * (members // 2) + position // 2
        back[s] = running.astype(BF16)
        factor = factors[s * rows : s * rows + 1] + factors[s * rows + 1 : s * rows + 2]
        running = running * factor + arrived[s, :, :width].astype(F32)


def squares_rows(squares):
    rows = squares.shape[0]
    lane = iota((rows, 128), 1)
    block = jnp.zeros((rows, 128), F32)
    for index, part in enumerate(split_bf16(squares, 3)):
        block = jnp.where(lane == index, part.astype(F32), block)
    return jnp.transpose(block)[:8]


def output_terms(base, ahead, maps, entering, gain, out_hbm, mine, given, out_w, out_sems):
    n = maps.shape[2] // 2
    count, _, width = mine.shape
    copies = fetch_columns(out_hbm, out_w, out_sems)
    rows = base.shape[1]
    scaled = []
    for m, term in enumerate((mine, given)):
        across = dot(maps[m, :, n:], entering[m])
        gated = base[m] + across * ahead[m]
        squares = jnp.sum(gated * gated, axis=1, keepdims=True)
        scaled.append((gated * gain[...]).astype(BF16))
        block = squares_rows(squares)
        block = jnp.concatenate([block, jnp.zeros((8, width - 128), F32)], 1).astype(term.dtype)
        for b in range(count):
            term[b, rows:] = block
    scaled = jnp.concatenate(scaled)
    for b in range(count):
        copies[b].wait()
        value = dot(scaled, out_w[:, b * width : (b + 1) * width])
        mine[b, :rows] = value[:rows].astype(mine.dtype)
        given[b, :rows] = value[rows:].astype(given.dtype)


def merge_cores(chip_ref, mine, arrived, kept, *sent):
    count, tall, width = mine.shape
    rows = tall - 8
    chip = chip_ref[0]
    kept[:rows] = mine[chip, :rows].astype(F32) + arrived[chip, :rows].astype(F32)
    both = jnp.sum(mine[0, rows:].astype(F32) + arrived[0, rows:].astype(F32), axis=0, keepdims=True)
    row = iota((8, width), 0)
    kept[rows:] = jnp.where(row == 0, both, 0.0)
    block = jnp.zeros((8, width), F32)
    for index, part in enumerate(split_bf16(both, 3)):
        block = jnp.where(row == index, part.astype(F32), block)
    for k in range(1, count):
        b = lax.rem(chip + k, count)
        sent[k - 1][:rows] = (mine[b, :rows].astype(F32) + arrived[b, :rows].astype(F32)).astype(BF16)
        sent[k - 1][rows:] = block.astype(BF16)


def finish(piece, kept, *refs):
    arrived, result = refs[:-1], refs[-1]
    rows = piece.shape[0]
    total = kept[:rows]
    squares = kept[rows:, :128]
    for part in arrived:
        total = total + part[:rows].astype(F32)
        squares = squares + part[rows:, :128].astype(F32)
    squares = jnp.broadcast_to(jnp.sum(squares, axis=0, keepdims=True), (rows, 128))
    scale = lax.rsqrt(jnp.transpose(squares) / INNER + EPS)
    for tile in range(piece.shape[1] // 128):
        span = slice(tile * 128, (tile + 1) * 128)
        result[:, span] = (piece[:, span].astype(F32) + scale * total[:, span]).astype(BF16)


def layer(piece, edge, weights):
    (
        prenorm,
        gate_weight,
        inner_weight,
        state_weight,
        step_weight,
        inner_taps,
        state_taps,
        step_bias,
        decay_rate,
        skip_scale,
        inner_gain,
        out_weight,
    ) = weights
    chip = lax.axis_index("chip").reshape(1)
    count = lax.axis_size("chip")
    members = lax.axis_size(SEQ)
    rows, block = piece.shape
    tall = 2 * rows
    width = inner_weight.shape[1]
    maps_width = state_weight.shape[1]
    heads = step_weight.shape[1]
    spread_rows = jnp.concatenate([edge, piece], axis=0)
    gain = prenorm.reshape(count, 1, block)
    steps_weight = step_weight.T

    def moved(step):
        return lax.ppermute(spread_rows, "chip", ring(count, step))

    far = moved(2)
    before = moved(1)
    after = moved(3)
    own = {0: spread_rows, 1: before, 2: far, 3: after}
    other = {k: lax.ppermute(part, "core", SWAP) for k, part in own.items()}
    near = [own[k] for k in NEAR] + [other[k] for k in NEAR]
    far = [own[k] for k in FAR] + [other[k] for k in FAR]
    high = 2 * spread_rows.shape[0]
    scaled, squares, *partial, state_rest, inner_rest = local(
        enter_near,
        [*near, gain, steps_weight, state_weight, inner_weight],
        [
            ((len(NEAR), high, block), BF16),
            ((high, 128), F32),
            ((high, heads), F32),
            ((high, maps_width), F32),
            ((high, width), F32),
            ((len(FAR) * block, maps_width), BF16),
            ((len(FAR) * block, width), BF16),
        ],
        weights=2,
        scratch=[
            *room(state_weight, len(NEAR), len(NEAR) * block),
            *room(inner_weight, len(NEAR), len(NEAR) * block),
            pltpu.SemaphoreType.DMA((len(FAR),)),
            pltpu.SemaphoreType.DMA((len(FAR),)),
        ],
    )
    scaled_far, scales, x, maps, steps, sums, sent = local(
        enter_far,
        [
            *far,
            squares,
            *partial,
            gain,
            steps_weight,
            inner_taps[:, None],
            state_taps[:, None],
            step_bias[None],
            decay_rate[None],
            state_rest,
            inner_rest,
        ],
        [
            ((len(FAR), high, block), BF16),
            ((tall, 128), F32),
            ((2, rows, width), BF16),
            ((2, rows, maps_width), BF16),
            ((2, rows, heads), F32),
            ((2, rows, heads), F32),
            ((tall, width + 128), BF16),
        ],
    )
    arrived = lax.all_to_all(sent.reshape(members, tall // members, -1), CROSS, 0, 0, tiled=True)
    (gate,) = local(
        gate_project,
        [scaled, scaled_far, scales, gate_weight],
        [((tall, width), F32)],
        weights=1,
        scratch=room(gate_weight, count),
    )
    base, ahead = local(
        local_mixing,
        [x, maps, steps, sums, gate, skip_scale[None]],
        [((2, rows, width), F32), ((2, rows, width), F32)],
    )
    (back,) = local(scan_states, [arrived], [((members, tall // members, width), BF16)])
    back = lax.all_to_all(back, CROSS, 0, 0, tiled=True)
    entering = back.reshape(2, rows, width)
    mine, given = local(
        output_terms,
        [base, ahead, maps, entering, inner_gain[None], out_weight],
        [((count, rows + 8, block), BF16)] * 2,
        weights=1,
        scratch=room(out_weight, count),
    )
    taken = lax.ppermute(given, "core", SWAP)
    kept, *leaving = local(
        merge_cores,
        [chip, mine, taken],
        [((rows + 8, block), F32)] + [((rows + 8, block), BF16)] * (count - 1),
        scalars=1,
    )
    parts = [lax.ppermute(part, "chip", ring(count, k + 1)) for k, part in enumerate(leaving)]
    return local(finish, [piece, kept, *parts], [((rows, block), BF16)])[0]


def shards(
    tokens,
    prenorm_gain,
    gate_weight,
    inner_weight,
    state_weight,
    step_weight,
    inner_taps,
    state_taps,
    step_bias,
    decay_rate,
    skip_scale,
    inner_gain,
    out_weight,
):
    weights = (
        prenorm_gain[0],
        gate_weight[0],
        inner_weight[0],
        state_weight[0],
        step_weight[0],
        inner_taps[0],
        state_taps[0],
        step_bias[0],
        decay_rate[0],
        skip_scale[0],
        inner_gain[0],
        out_weight[0],
    )
    sections = lax.axis_size("pipe")
    section = lax.axis_index("pipe")
    core = lax.axis_index("core")
    width = tokens.shape[2]
    members = lax.axis_size(SEQ)
    edges = lax.ppermute(tokens[:, -EDGE:], SEQ, [(s, s + 1) for s in range(members - 1)])
    rows = jnp.concatenate([edges, tokens], axis=1)
    mine = jnp.where(core == 0, rows[0], rows[1])
    given = lax.ppermute(jnp.where(core == 0, rows[1], rows[0]), "core", SWAP)

    def joined(left, right):
        return jnp.where(
            core == 0, jnp.concatenate([left, right], 1), jnp.concatenate([right, left], 1)
        )

    joint = joined(mine, given)
    piece, edge = joint[EDGE:], joint[:EDGE]
    kept = None
    for turn in range(sections):
        own = layer(piece, edge, weights)
        kept = own if turn == 0 else jnp.where(section == turn, own, kept)
        if turn + 1 < sections:
            piece = lax.ppermute(own, "pipe", [(s, s + 1) for s in range(sections - 1)])
            edge = lax.ppermute(
                own[-EDGE:],
                ("pipe", *SEQ),
                [
                    (p * members + s, (p + 1) * members + s + 1)
                    for p in range(sections - 1)
                    for s in range(members - 1)
                ],
            )
    left, right = kept[:, :width], kept[:, width:]
    held = jnp.where(core == 0, left, right)
    given = lax.ppermute(jnp.where(core == 0, right, left), "core", SWAP)
    return jnp.where(core == 0, jnp.stack([held, given]), jnp.stack([given, held]))[None]


def solution(mesh):
    torus = Mesh(
        mesh.devices.reshape(mesh.shape["pipe"], mesh.shape["tensor"] // 2, 2, 8, 2),
        ("pipe", "chip", "core", "seq_0", "seq_1"),
    )
    return jax.shard_map(
        shards,
        mesh=torus,
        in_specs=(
            P(None, SEQ, TENSOR),
            P("pipe", None),
            P("pipe", None, TENSOR),
            P("pipe", None, TENSOR),
            P("pipe", None, None),
            P("pipe", None, TENSOR),
            P("pipe", None, TENSOR),
            P("pipe", None, None),
            P("pipe", TENSOR),
            P("pipe", TENSOR),
            P("pipe", TENSOR),
            P("pipe", TENSOR),
            P("pipe", TENSOR, None),
        ),
        out_specs=P("pipe", None, SEQ, TENSOR),
        check_vma=False,
    )
```

```python
import jax
import jax.numpy as jnp
from jax import lax
from jax.experimental import pallas as pl
from jax.experimental.pallas import tpu as pltpu
from jax.sharding import Mesh
from jax.sharding import PartitionSpec as P

INNER = 5120
EPS = 1e-05
EDGE = 8
NEAR = (0,)
FAR = (2, 1, 3)
LEAVING = (2, 1, 3, 0)
SEQ = ("seq_0", "seq_1")
CROSS = ("seq_1", "seq_0")
TENSOR = ("chip", "core")
SWAP = [(0, 1), (1, 0)]
F32 = jnp.float32
BF16 = jnp.bfloat16
VMEM = pl.BlockSpec(memory_space=pltpu.VMEM)
SMEM = pl.BlockSpec(memory_space=pltpu.SMEM)
HBM = pl.BlockSpec(memory_space=pltpu.MemorySpace.HBM)


def ring(size, steps):
    return [(source, (source + steps) % size) for source in range(size)]


def split_bf16(value, count):
    parts = []
    for _ in range(count):
        part = value.astype(BF16)
        parts.append(part)
        value = value - part.astype(F32)
    return parts


def local(body, args, outs, scalars=0, weights=0, scratch=(), mib=16, flops=1 << 28):
    first = len(args) - weights
    args = [
        pltpu.with_memory_space_constraint(arg, pltpu.MemorySpace.HBM) if index >= first else arg
        for index, arg in enumerate(args)
    ]
    return pl.pallas_call(
        body,
        out_shape=[jax.ShapeDtypeStruct(shape, kind) for shape, kind in outs],
        in_specs=[SMEM] * scalars + [VMEM] * (len(args) - scalars - weights) + [HBM] * weights,
        out_specs=[VMEM] * len(outs),
        cost_estimate=pl.CostEstimate(flops=flops, transcendentals=0, bytes_accessed=1 << 22),
        scratch_shapes=list(scratch),
        compiler_params=pltpu.CompilerParams(vmem_limit_bytes=mib << 20),
    )(*args)


def fetch(source, target, semaphores, blocks=None):
    parts = semaphores.shape[0]
    size = target.shape[0] // parts
    copies = [
        pltpu.make_async_copy(
            source.at[pl.ds((part if blocks is None else blocks[part]) * size, size)],
            target.at[pl.ds(part * size, size)],
            semaphores.at[part],
        )
        for part in range(parts)
    ]
    for copy in copies:
        copy.start()
    return copies


def blocks_of(steps):
    chip, count = lax.axis_index("chip"), 4
    return [lax.rem(chip - step + count, count) for step in steps]


def fetch_columns(source, target, semaphores, blocks):
    parts = semaphores.shape[0]
    size = target.shape[1] // parts
    copies = [
        pltpu.make_async_copy(
            source.at[:, pl.ds(blocks[part] * size, size)],
            target.at[:, pl.ds(part * size, size)],
            semaphores.at[part],
        )
        for part in range(parts)
    ]
    for copy in copies:
        copy.start()
    return copies


def room(weight, parts, rows=None):
    shape = (rows or weight.shape[0], weight.shape[1])
    return [pltpu.VMEM(shape, weight.dtype), pltpu.SemaphoreType.DMA((parts,))]


def dot(a, b, dims=((1,), (0,))):
    return lax.dot_general(a, b, (dims, ((), ())), preferred_element_type=F32)


def sigmoid(value):
    return 1.0 / (1.0 + jnp.exp(-value))


def iota(shape, dim):
    return lax.broadcasted_iota(jnp.int32, shape, dim)


def spread(heads, width, copies=1):
    size = width // heads
    lane, head = iota((heads * copies, width), 1), iota((heads * copies, width), 0) % heads
    return jnp.where((lane >= head * size) & (lane < (head + 1) * size), 1.0, 0.0).astype(BF16)


def over_channels(value, width):
    parts = [part.astype(F32) for part in split_bf16(value, 3)]
    return dot(jnp.concatenate(parts, 1).astype(BF16), spread(value.shape[1], width, 3))


def convolve(rim, values, taps):
    width = taps.shape[0] - 1
    length = values.shape[0]
    padded = jnp.concatenate([rim, values], axis=0).astype(F32)
    lead = rim.shape[0] - width + 1
    total = taps[width]
    for index in range(width):
        total = total + taps[index] * padded[lead + index : lead + index + length]
    return (total * sigmoid(total)).astype(BF16)


def place(piece, gain, scaled, side, edge):
    rows = piece.shape[0] - edge
    value = piece[...].astype(F32)
    square = value * value
    squares = 0.0
    for tile in range(piece.shape[1] // 128):
        squares = squares + square[:, tile * 128 : (tile + 1) * 128]
    value = value * gain
    scaled[side * rows : (side + 1) * rows, :] = value[edge:].astype(BF16)
    return squares, value[:edge]


def columns(array, b, width):
    return array[:, pl.ds(pl.multiple_of(b * width, width), width)]


def multiply(scaled, part, step_w, state_w, inner_w, copies):
    block = scaled.shape[1]
    span = slice(part * block, (part + 1) * block)
    value = scaled[...]
    step = dot(value, step_w, ((1,), (1,)))
    if copies is not None:
        copies[0][part].wait()
    state = dot(value, state_w[span, :])
    if copies is not None:
        copies[1][part].wait()
    return step, state, dot(value, inner_w[span, :])


def enter_near(*refs):
    count = len(NEAR)
    sides = refs[:count], refs[count : 2 * count]
    gain, step_w, state_hbm, inner_hbm = refs[2 * count :][:4]
    scaled, squares, step, state, inner, state_rest, inner_rest = refs[2 * count + 4 :][:7]
    state_w, state_sems, inner_w, inner_sems, state_rest_sems, inner_rest_sems = refs[
        2 * count + 11 :
    ]
    blocks = blocks_of(NEAR)
    copies = fetch(state_hbm, state_w, state_sems, blocks), fetch(
        inner_hbm, inner_w, inner_sems, blocks
    )
    rest = fetch(state_hbm, state_rest, state_rest_sems, blocks_of(FAR))
    rest += fetch(inner_hbm, inner_rest, inner_rest_sems, blocks_of(FAR))
    edge = EDGE
    rows = sides[0][0].shape[0] - edge
    width = sides[0][0].shape[1]
    sums = [0.0, 0.0]
    totals = [0.0, 0.0, 0.0]
    for k, b in enumerate(blocks):
        tails = []
        for side in range(2):
            part, tail = place(sides[side][k], gain[b], scaled.at[k], side, edge)
            sums[side] = sums[side] + part
            tails.append(tail)
        scaled[k, 2 * rows :, :] = jnp.concatenate(tails).astype(BF16)
        parts = multiply(scaled.at[k], k, columns(step_w, b, width), state_w, inner_w, copies)
        totals = [total + part for total, part in zip(totals, parts)]
    for side in range(2):
        squares[side * rows : (side + 1) * rows, :] = sums[side][edge:]
        squares[2 * rows + side * edge : 2 * rows + (side + 1) * edge, :] = sums[side][:edge]
    step[...], state[...], inner[...] = totals
    for copy in rest:
        copy.wait()


def enter_far(*refs):
    count = len(FAR)
    sides = refs[:count], refs[count : 2 * count]
    squares_in, step_in, state_in, inner_in = refs[2 * count :][:4]
    refs = refs[2 * count + 4 :]
    gain, step_w, inner_taps, state_taps, bias, rate, state_w, inner_w = refs[:8]
    scaled, scales, x, maps, steps, sums, sent = refs[8:]
    blocks = blocks_of(FAR)
    edge = EDGE
    rows, width = x.shape[1:]
    block = sides[0][0].shape[1]
    heads = bias.shape[1]
    n = maps.shape[2] // 2
    found = [0.0, 0.0]
    for k, b in enumerate(blocks):
        tails = []
        for side in range(2):
            part, tail = place(sides[side][k], gain[b], scaled.at[k], side, edge)
            found[side] = found[side] + part
            tails.append(tail)
        scaled[k, 2 * rows :, :] = jnp.concatenate(tails).astype(BF16)
    found = jnp.concatenate([found[0][edge:], found[1][edge:], found[0][:edge], found[1][:edge]])
    squares = jnp.sum(squares_in[...] + found, axis=1, keepdims=True)
    scale = lax.rsqrt(squares / (len(NEAR + FAR) * block) + EPS)
    scales[...] = jnp.broadcast_to(scale[: 2 * rows], scales.shape)
    totals = [step_in[...], state_in[...], inner_in[...]]
    for k, b in enumerate(blocks):
        parts = multiply(scaled.at[k], k, columns(step_w, b, block), state_w, inner_w, None)
        totals = [total + part for total, part in zip(totals, parts)]
    step, state, inner = totals
    raw = (step * scale)[: 2 * rows] + bias[...]
    step_all = jnp.maximum(raw, 0.0) + jnp.log1p(jnp.exp(-jnp.abs(raw)))
    state = (state * scale).astype(BF16).astype(F32)
    inner = (inner * scale).astype(BF16).astype(F32)
    lower = (iota((rows, rows), 0) >= iota((rows, rows), 1)).astype(BF16)
    for m in range(2):
        span = slice(m * rows, (m + 1) * rows)
        ends = slice(2 * rows + m * edge, 2 * rows + (m + 1) * edge)
        sm = convolve(state[ends], state[span], state_taps)
        xm = convolve(inner[ends], inner[span], inner_taps)
        x[m] = xm
        maps[m] = sm
        step = step_all[span]
        total = -sum(dot(lower, part) for part in split_bf16(step * rate[...], 3))
        last = total[rows - 1 :]
        steps[m] = step
        sums[m] = total
        weighting = over_channels(jnp.exp(last - total) * step, width)
        weighted = (xm.astype(F32) * weighting).astype(BF16)
        sent[span, :width] = dot(sm[:, :n], weighted, ((0,), (0,))).astype(BF16)
        high, low = split_bf16(jnp.exp(last), 2)
        row = iota((rows, heads), 0) % 16
        ends = jnp.where(row == 0, high.astype(F32), low.astype(F32))
        ends = jnp.concatenate([ends, jnp.zeros((rows, sent.shape[1] - width - heads), F32)], 1)
        sent[span, width:] = ends.astype(BF16)


def gate_project(near, far, scales, gate_hbm, gate, gate_w, gate_sems):
    copies = fetch(gate_hbm, gate_w, gate_sems, blocks_of(NEAR + FAR))
    rows, width = gate.shape
    block = far.shape[2]
    total = 0.0
    for part in range(len(NEAR + FAR)):
        scaled = near[part, :rows] if part < len(NEAR) else far[part - len(NEAR), :rows]
        copies[part].wait()
        total = total + dot(scaled, gate_w[part * block : (part + 1) * block, :])
    for tile in range(width // 128):
        span = slice(tile * 128, (tile + 1) * 128)
        value = (total[:, span] * scales[...]).astype(BF16).astype(F32)
        gate[:, span] = value * sigmoid(value)


def local_mixing(x, maps, steps, sums, gate, skip, base, ahead):
    micros, rows, width = x.shape
    heads = skip.shape[1]
    size = width // heads
    pair = 128 // size
    n = maps.shape[2] // 2
    skips = over_channels(jnp.broadcast_to(skip[...], (8, heads)), width)[:1]
    later = iota((rows, rows), 0) >= iota((rows, rows), 1)
    lane = iota((rows, pair * size), 1)
    for m in range(micros):
        maps_m, sums_m, steps_m = maps[m], sums[m], steps[m]
        scores = dot(maps_m[:, n:], maps_m[:, :n], ((1,), (1,)))
        fill = jnp.zeros((rows, 128 - heads), F32)
        sums_t = jnp.transpose(jnp.concatenate([sums_m, fill], 1))
        steps_t = jnp.transpose(jnp.concatenate([steps_m, fill], 1))
        for g in range(heads // pair):
            span = slice(g * pair * size, (g + 1) * pair * size)
            xg = x[m, :, span]
            left, right = [], []
            for j in range(pair):
                h = g * pair + j
                gap = sums_m[:, h : h + 1] - sums_t[h : h + 1, :]
                decay = jnp.exp(jnp.where(later, gap, -jnp.inf))
                left.append((scores * decay * steps_t[h : h + 1, :]).astype(BF16))
                right.append(
                    jnp.where((lane >= j * size) & (lane < (j + 1) * size), xg, jnp.zeros_like(xg))
                )
            inside = dot(jnp.concatenate(left, 1), jnp.concatenate(right, 0))
            silu = gate[m * rows : (m + 1) * rows, span]
            base[m, :, span] = (inside + skips[:, span] * xg.astype(F32)) * silu
        ahead[m] = over_channels(jnp.exp(sums_m), width) * gate[m * rows : (m + 1) * rows]


def scan_states(arrived, back, heads=10):
    members, rows, width = back.shape
    picks = spread(128, 128 * (width // heads))[:, :width]
    ends = arrived[:, :, width:].reshape(members * rows, arrived.shape[2] - width)
    factors = dot(ends, picks)
    running = jnp.zeros((rows, width), F32)
    for position in range(members):
        s = position % 2 * (members // 2) + position // 2
        back[s] = running.astype(BF16)
        factor = factors[s * rows : s * rows + 1] + factors[s * rows + 1 : s * rows + 2]
        running = running * factor + arrived[s, :, :width].astype(F32)


def squares_rows(squares):
    rows = squares.shape[0]
    lane = iota((rows, 128), 1)
    block = jnp.zeros((rows, 128), F32)
    for index, part in enumerate(split_bf16(squares, 3)):
        block = jnp.where(lane == index, part.astype(F32), block)
    return jnp.transpose(block)[:8]


def output_terms(base, ahead, maps, entering, gain, out_hbm, *refs):
    count = len(LEAVING)
    mine, given, (out_w, out_sems) = refs[:count], refs[count : 2 * count], refs[2 * count :]
    n = maps.shape[2] // 2
    width = mine[0].shape[1]
    copies = fetch_columns(out_hbm, out_w, out_sems, blocks_of([-step for step in LEAVING]))
    rows = base.shape[1]
    scaled = []
    for m, terms in enumerate((mine, given)):
        across = dot(maps[m, :, n:], entering[m])
        gated = base[m] + across * ahead[m]
        squares = jnp.sum(gated * gated, axis=1, keepdims=True)
        scaled.append((gated * gain[...]).astype(BF16))
        block = squares_rows(squares)
        block = jnp.concatenate([block, jnp.zeros((8, width - 128), F32)], 1).astype(BF16)
        for term in terms:
            term[rows:] = block
    scaled = jnp.concatenate(scaled)
    for part in range(count):
        copies[part].wait()
        value = dot(scaled, out_w[:, part * width : (part + 1) * width]).astype(BF16)
        mine[part][:rows] = value[:rows]
        given[part][:rows] = value[rows:]


def merge_cores(mine, arrived, merged):
    width = mine.shape[1]
    rows = mine.shape[0] - 8
    total = mine[...].astype(F32) + arrived[...].astype(F32)
    merged[:rows] = total[:rows].astype(merged.dtype)
    both = jnp.sum(total[rows:], axis=0, keepdims=True)
    row = iota((8, width), 0)
    block = jnp.zeros((8, width), F32)
    for index, part in enumerate(split_bf16(both, 3)):
        block = jnp.where(row == index, part.astype(F32), block)
    merged[rows:] = block.astype(merged.dtype)


def finish(piece, kept, *refs):
    arrived, result = refs[:-1], refs[-1]
    rows = piece.shape[0]
    total = kept[:rows]
    squares = kept[rows:, :128]
    for part in arrived:
        total = total + part[:rows].astype(F32)
        squares = squares + part[rows:, :128].astype(F32)
    squares = jnp.broadcast_to(jnp.sum(squares, axis=0, keepdims=True), (rows, 128))
    scale = lax.rsqrt(jnp.transpose(squares) / INNER + EPS)
    for tile in range(piece.shape[1] // 128):
        span = slice(tile * 128, (tile + 1) * 128)
        result[:, span] = (piece[:, span].astype(F32) + scale * total[:, span]).astype(BF16)


def layer(piece, edge, weights):
    (
        prenorm,
        gate_weight,
        inner_weight,
        state_weight,
        step_weight,
        inner_taps,
        state_taps,
        step_bias,
        decay_rate,
        skip_scale,
        inner_gain,
        out_weight,
    ) = weights
    count = lax.axis_size("chip")
    members = lax.axis_size(SEQ)
    rows, block = piece.shape
    tall = 2 * rows
    width = inner_weight.shape[1]
    maps_width = state_weight.shape[1]
    heads = step_weight.shape[1]
    spread_rows = jnp.concatenate([edge, piece], axis=0)
    gain = prenorm.reshape(count, 1, block)
    steps_weight = step_weight.T

    def moved(step):
        return lax.ppermute(spread_rows, "chip", ring(count, step))

    far = moved(2)
    before = moved(1)
    after = moved(3)
    own = {0: spread_rows, 1: before, 2: far, 3: after}
    other = {k: lax.ppermute(part, "core", SWAP) for k, part in own.items()}
    near = [own[k] for k in NEAR] + [other[k] for k in NEAR]
    far = [own[k] for k in FAR] + [other[k] for k in FAR]
    high = 2 * spread_rows.shape[0]
    scaled, squares, *partial, state_rest, inner_rest = local(
        enter_near,
        [*near, gain, steps_weight, state_weight, inner_weight],
        [
            ((len(NEAR), high, block), BF16),
            ((high, 128), F32),
            ((high, heads), F32),
            ((high, maps_width), F32),
            ((high, width), F32),
            ((len(FAR) * block, maps_width), BF16),
            ((len(FAR) * block, width), BF16),
        ],
        weights=2,
        scratch=[
            *room(state_weight, len(NEAR), len(NEAR) * block),
            *room(inner_weight, len(NEAR), len(NEAR) * block),
            pltpu.SemaphoreType.DMA((len(FAR),)),
            pltpu.SemaphoreType.DMA((len(FAR),)),
        ],
    )
    scaled_far, scales, x, maps, steps, sums, sent = local(
        enter_far,
        [
            *far,
            squares,
            *partial,
            gain,
            steps_weight,
            inner_taps[:, None],
            state_taps[:, None],
            step_bias[None],
            decay_rate[None],
            state_rest,
            inner_rest,
        ],
        [
            ((len(FAR), high, block), BF16),
            ((tall, 128), F32),
            ((2, rows, width), BF16),
            ((2, rows, maps_width), BF16),
            ((2, rows, heads), F32),
            ((2, rows, heads), F32),
            ((tall, width + 128), BF16),
        ],
    )
    arrived = lax.all_to_all(sent.reshape(members, tall // members, -1), CROSS, 0, 0, tiled=True)
    (gate,) = local(
        gate_project,
        [scaled, scaled_far, scales, gate_weight],
        [((tall, width), F32)],
        weights=1,
        scratch=room(gate_weight, count),
    )
    base, ahead = local(
        local_mixing,
        [x, maps, steps, sums, gate, skip_scale[None]],
        [((2, rows, width), F32), ((2, rows, width), F32)],
    )
    (back,) = local(scan_states, [arrived], [((members, tall // members, width), BF16)])
    back = lax.all_to_all(back, CROSS, 0, 0, tiled=True)
    entering = back.reshape(2, rows, width)
    terms = local(
        output_terms,
        [base, ahead, maps, entering, inner_gain[None], out_weight],
        [((rows + 8, block), BF16)] * (2 * count),
        weights=1,
        scratch=room(out_weight, count),
    )
    parts = []
    for step, mine, given in zip(LEAVING, terms[:count], terms[count:]):
        kind = BF16 if step else F32
        (part,) = local(
            merge_cores,
            [mine, lax.ppermute(given, "core", SWAP)],
            [((rows + 8, block), kind)],
        )
        parts.append(lax.ppermute(part, "chip", ring(count, step)) if step else part)
    kept = parts.pop()
    return local(finish, [piece, kept, *parts], [((rows, block), BF16)])[0]


def shards(
    tokens,
    prenorm_gain,
    gate_weight,
    inner_weight,
    state_weight,
    step_weight,
    inner_taps,
    state_taps,
    step_bias,
    decay_rate,
    skip_scale,
    inner_gain,
    out_weight,
):
    weights = (
        prenorm_gain[0],
        gate_weight[0],
        inner_weight[0],
        state_weight[0],
        step_weight[0],
        inner_taps[0],
        state_taps[0],
        step_bias[0],
        decay_rate[0],
        skip_scale[0],
        inner_gain[0],
        out_weight[0],
    )
    sections = lax.axis_size("pipe")
    section = lax.axis_index("pipe")
    core = lax.axis_index("core")
    width = tokens.shape[2]
    members = lax.axis_size(SEQ)
    edges = lax.ppermute(tokens[:, -EDGE:], SEQ, [(s, s + 1) for s in range(members - 1)])
    rows = jnp.concatenate([edges, tokens], axis=1)
    mine = jnp.where(core == 0, rows[0], rows[1])
    given = lax.ppermute(jnp.where(core == 0, rows[1], rows[0]), "core", SWAP)

    def joined(left, right):
        return jnp.where(
            core == 0, jnp.concatenate([left, right], 1), jnp.concatenate([right, left], 1)
        )

    joint = joined(mine, given)
    piece, edge = joint[EDGE:], joint[:EDGE]
    kept = None
    for turn in range(sections):
        own = layer(piece, edge, weights)
        kept = own if turn == 0 else jnp.where(section == turn, own, kept)
        if turn + 1 < sections:
            piece = lax.ppermute(own, "pipe", [(s, s + 1) for s in range(sections - 1)])
            edge = lax.ppermute(
                own[-EDGE:],
                ("pipe", *SEQ),
                [
                    (p * members + s, (p + 1) * members + s + 1)
                    for p in range(sections - 1)
                    for s in range(members - 1)
                ],
            )
    left, right = kept[:, :width], kept[:, width:]
    held = jnp.where(core == 0, left, right)
    given = lax.ppermute(jnp.where(core == 0, right, left), "core", SWAP)
    return jnp.where(core == 0, jnp.stack([held, given]), jnp.stack([given, held]))[None]


def solution(mesh):
    torus = Mesh(
        mesh.devices.reshape(mesh.shape["pipe"], mesh.shape["tensor"] // 2, 2, 8, 2),
        ("pipe", "chip", "core", "seq_0", "seq_1"),
    )
    return jax.shard_map(
        shards,
        mesh=torus,
        in_specs=(
            P(None, SEQ, TENSOR),
            P("pipe", None),
            P("pipe", None, TENSOR),
            P("pipe", None, TENSOR),
            P("pipe", None, None),
            P("pipe", None, TENSOR),
            P("pipe", None, TENSOR),
            P("pipe", None, None),
            P("pipe", TENSOR),
            P("pipe", TENSOR),
            P("pipe", TENSOR),
            P("pipe", TENSOR),
            P("pipe", TENSOR, None),
        ),
        out_specs=P("pipe", None, SEQ, TENSOR),
        check_vma=False,
    )
```
